32 devices in a mesh: pair: 2 (over core), dp: 16 (over z, y, x).
Axes of the slice: x: 2, y: 2, z: 4, core: 2. Of those that a mesh axis runs over, the one named last changes fastest.
Arguments:
- inputs: bfloat16 [2, 32, 512, 768], P('pair', 'dp'), may hold values from -6 to 6
- cotangent: bfloat16 [2, 32, 512, 768], P('pair', 'dp'), may hold values from -6 to 6
- span_lengths: int32 [2, 32, 4], P('pair', 'dp'), may hold values from 64 to 320, as said below
- pad_lengths: int32 [2, 32], P('pair', 'dp'), may hold values from 0 to 128, as said below
- pairing: int32 [2, 16, 8], P('pair', 'dp'), may hold values from 0 to 7, as said below
- owner_slot: int32 [108], replicated, may hold values from 0 to 111, as said below
- master: float32 [112, 256, 256], P('dp'), as said below
- first_moment: float32 [112, 256, 256], P('dp'), may hold values from -4 to 4
- second_moment: float32 [112, 256, 256], P('dp'), may hold values from 0.16 to 16
- left_basis: float32 [112, 256, 256], P('dp'), may hold values from -1 to 1
- right_basis: float32 [112, 256, 256], P('dp'), may hold values from -1 to 1
- vector_master: float32 [9216], replicated
- vector_first: float32 [9216], replicated, may hold values from -4 to 4
- vector_second: float32 [9216], replicated, may hold values from 0.16 to 16
Outputs:
- block_output: bfloat16 [2, 32, 512, 768], P('pair', 'dp')
- input_grad: float32 [2, 32, 512, 768], P('pair', 'dp')
- weight_grad: float32 [112, 256, 256], P('dp')
- new_master: float32 [112, 256, 256], P('dp')
- new_first: float32 [112, 256, 256], P('dp')
- new_second: float32 [112, 256, 256], P('dp')
- vector_grad: float32 [9216], replicated
- vector_state: float32 [3, 9216], replicated
The draws below stay inside these ranges and needn't reach their ends.
Inputs may be any that keep to these rules, and one draw needn't show every extreme that they name: `span_lengths`: each row's spans come first in order and each has 64 tokens or more; the row's padding follows them; some span has exactly 320 tokens. `pad_lengths`: equals 512 minus the sum of the row's span lengths; some row has exactly 128, some row has none. For each dp index, pairing[0] is a permutation of the 8 spans of the partner device and pairing[1] is its inverse; spans are numbered row by row. `owner_slot`: distinct values; slot p belongs to dp index p // 7; every dp index holds at most 7 blocks and some hold exactly 7. `master`: slots that no block uses hold values that take part in no output but their own update.
All inputs are finite; a program needn't handle non-finite values.
Results may differ from the reference program's by a relative error of at most 0.012.
Values may be sent and summed in bfloat16 or wider, within the bound.
A program may use at most 256 MiB of HBM per device.

```python
import math
import jax
import jax.numpy as jnp
from jax import lax

D = 768
HEADS = 12
HEAD_DIM = 64
FF = 3072
LEN = 512
SEGS = 4
MINSPAN = 64
PADMAX = 128
BLOCK = 256
STEP = 10
ROWS_DEV = 2
ROWS = 32
NSEG = 8
NB = 108
SLOTS = 7
PV = 9216
GRAD_SQ = 32
N_PAIR = 2
N_DP = 16


def owner_table(key):
    lower_count = (N_DP - 1) * SLOTS
    chosen = jax.random.permutation(jax.random.fold_in(key, 101), lower_count)[:NB - SLOTS].astype(jnp.int32)
    top_slots = jnp.arange(lower_count, N_DP * SLOTS, dtype=jnp.int32)
    every_slot = jnp.concatenate([chosen, top_slots], axis=0)
    shuffle_order = jax.random.permutation(jax.random.fold_in(key, 103), NB)
    return every_slot[shuffle_order].astype(jnp.int32)


def draw_owner_slot(key, part):
    return owner_table(key)


def draw_master(key, part):
    owners = owner_table(key)
    block_of = jnp.full((N_DP * SLOTS,), -1, jnp.int32).at[owners].set(jnp.arange(NB, dtype=jnp.int32))
    square = D // BLOCK * (D // BLOCK)
    wide_count = D // BLOCK * (FF // BLOCK)
    narrow_spread = 1.0 / math.sqrt(D)
    spread = jnp.where(block_of < 3 * square, narrow_spread, jnp.where(block_of < 4 * square, 3.0 * narrow_spread, jnp.where(block_of < 4 * square + wide_count, narrow_spread, 1.0 / math.sqrt(FF))))
    grid_shape = (N_DP * SLOTS, BLOCK, BLOCK)
    values = jax.random.normal(jax.random.fold_in(key, 102), grid_shape, jnp.float32)
    return values * spread[:, None, None].astype(jnp.float32)


def basis_draw(key, salt):
    count = N_DP * SLOTS
    key_list = jax.random.split(jax.random.fold_in(key, salt), count)
    orders = jax.vmap(lambda single: jax.random.permutation(single, BLOCK))(key_list).astype(jnp.int32)
    sign_flip = 2 * jax.random.randint(jax.random.fold_in(key, salt + 1), (count, BLOCK), 0, 2) - 1
    column = jnp.arange(BLOCK, dtype=jnp.int32)
    phase_index = (2 * column[None, None, :] + 1) * orders[:, :, None] % (4 * BLOCK)
    amplitude = jnp.where(orders == 0, math.sqrt(1.0 / BLOCK), math.sqrt(2.0 / BLOCK)).astype(jnp.float32)
    basis_table = amplitude[:, :, None] * jnp.cos(phase_index.astype(jnp.float32) * (math.pi / (2 * BLOCK))) * sign_flip[:, :, None].astype(jnp.float32)
    return basis_table


def draw_left_basis(key, part):
    return basis_draw(key, 401)


def draw_right_basis(key, part):
    return basis_draw(key, 501)


def draw_pairing(key, part):
    key_list = jax.random.split(jax.random.fold_in(key, 201), N_DP)
    orders = jax.vmap(lambda single: jax.random.permutation(single, NSEG))(key_list).astype(jnp.int32)
    inverse = jnp.argsort(orders, axis=-1, stable=True).astype(jnp.int32)
    return jnp.stack([orders, inverse], axis=0)


def span_table(key):
    grid_shape = (N_PAIR, ROWS)
    row_total = N_PAIR * ROWS
    pad_rows = jax.random.randint(jax.random.fold_in(key, 301), grid_shape, 0, PADMAX + 1)
    forced = jax.random.randint(jax.random.fold_in(key, 302), (), 0, row_total)
    other = (forced + 1 + jax.random.randint(jax.random.fold_in(key, 304), (), 0, row_total - 1)) % row_total
    pad_rows = pad_rows.reshape(-1).at[forced].set(PADMAX).at[other].set(0).reshape(grid_shape).astype(jnp.int32)
    remaining = LEN - pad_rows - SEGS * MINSPAN
    cut_points = jax.random.randint(jax.random.fold_in(key, 303), grid_shape + (SEGS - 1,), 0, 1 << 20) % (remaining[..., None] + 1)
    is_other = (jnp.arange(row_total, dtype=jnp.int32) == other).reshape(grid_shape)
    cut_points = jnp.where(is_other[..., None], 0, cut_points)
    cut_points = jnp.sort(cut_points, axis=-1)
    boundary = jnp.concatenate([jnp.zeros(grid_shape + (1,), jnp.int32), cut_points.astype(jnp.int32), remaining[..., None].astype(jnp.int32)], axis=-1)
    span_rows = boundary[..., 1:] - boundary[..., :-1] + MINSPAN
    return (span_rows.astype(jnp.int32), pad_rows)


def draw_span_lengths(key, part):
    return span_table(key)[0]


def draw_pad_lengths(key, part):
    return span_table(key)[1]


def draw_vector_master(key, part):
    position = jnp.arange(8 * D + FF)
    is_gain = (position < D) | (position >= 2 * D) & (position < 3 * D)
    jitter = jax.random.normal(jax.random.fold_in(key, 601), (8 * D + FF,), jnp.float32)
    return jnp.where(is_gain, 1.0 + 0.1 * jitter, 0.1 * jitter).astype(jnp.float32)


def block_levels(rng, extent, cuts, least, top_value):
    loudness = 1.0
    for dim, blocks in cuts:
        draws = jax.random.uniform(jax.random.fold_in(jax.random.fold_in(rng, 6), dim), (blocks,), jnp.float32, least / len(cuts), top_value / len(cuts))
        loudness = loudness * jnp.repeat(jnp.exp(draws), extent[dim] // blocks).reshape((-1,) + (1,) * (len(extent) - 1 - dim))
    return loudness


def centred(stream_key, dims, scale, bound, cuts=(), kind=jnp.bfloat16):
    values = scale * jax.random.normal(stream_key, dims, jnp.float32)
    if cuts:
        values = values * block_levels(stream_key, dims, cuts, -0.22, 0.18)
    return jnp.clip(values, -bound, bound).astype(kind)


def setup_inputs(seed: int = 0) -> dict:
    keys = jax.random.split(jax.random.key(seed), 15)
    inputs = centred(keys[0], (N_PAIR, ROWS, LEN, D), 1.0, 6.0, ((0, 2), (1, 16)))
    cotangent = centred(keys[1], (N_PAIR, ROWS, LEN, D), 1.0, 6.0, ((0, 2), (1, 16)))
    span_lengths = draw_span_lengths(jax.random.fold_in(keys[14], 71), 0)
    pad_lengths = draw_pad_lengths(jax.random.fold_in(keys[14], 71), 0)
    pairing = draw_pairing(jax.random.fold_in(keys[14], 71), 0)
    owner_slot = draw_owner_slot(jax.random.fold_in(keys[14], 71), 0)
    master = draw_master(jax.random.fold_in(keys[14], 71), 0)
    first_moment = centred(keys[7], (N_DP * SLOTS, BLOCK, BLOCK), (0.1 * GRAD_SQ ** 0.5), 4.0, ((0, 16),), jnp.float32)
    second_moment = jnp.clip(jnp.exp(math.log(16.0) - 4.6051702 * jax.random.uniform(keys[8], (N_DP * SLOTS, BLOCK, BLOCK), jnp.float32) ** block_levels(keys[8], (N_DP * SLOTS, BLOCK, BLOCK), ((0, 16),), -0.2, 0.2)), 0.16, 16.0)
    left_basis = draw_left_basis(jax.random.fold_in(keys[14], 71), 0)
    right_basis = draw_right_basis(jax.random.fold_in(keys[14], 71), 0)
    vector_master = draw_vector_master(jax.random.fold_in(keys[14], 71), 0)
    vector_first = centred(keys[12], (PV,), (0.1 * GRAD_SQ ** 0.5), 4.0, (), jnp.float32)
    vector_second = jnp.clip(jnp.exp(jax.random.uniform(keys[13], (PV,), jnp.float32, math.log(0.16), math.log(16.0))), 0.16, 16.0)
    return dict(inputs=inputs, cotangent=cotangent, span_lengths=span_lengths, pad_lengths=pad_lengths, pairing=pairing, owner_slot=owner_slot, master=master, first_moment=first_moment, second_moment=second_moment, left_basis=left_basis, right_basis=right_basis, vector_master=vector_master, vector_first=vector_first, vector_second=vector_second)


@jax.custom_vjp
def low(v):
    return lax.optimization_barrier(v.astype(jnp.bfloat16)).astype(jnp.float32)

@jax.custom_vjp
def low_back(v):
    return v

def low_keep(v):
    return (low(v), None)

def low_pass(kept, grad):
    return (grad,)

def back_keep(v):
    return (v, None)

def back_low(kept, grad):
    return (low(grad),)
low.defvjp(low_keep, low_pass)
low_back.defvjp(back_keep, back_low)
HIGHEST = lax.Precision.HIGHEST
BETA_ONE = 0.9
BETA_TWO = 0.95
ADAM_EPS = 1e-08
LR_MATRIX = 0.1
LR_VECTOR = 1.0
DECAY_RATE = 0.01
NORM_EPS = 1e-12
CLS_SCALE = 0.0625
CLS_WEIGHT = 4.0

def product(left_side, right_side):
    return jnp.dot(left_side, right_side, precision=HIGHEST, preferred_element_type=jnp.float32)

def layer_norm(values, gain_vector, shift_vector):
    average = lax.optimization_barrier(jnp.mean(values, axis=-1, keepdims=True))
    centered = values - average
    variance = lax.optimization_barrier(jnp.mean(centered * centered, axis=-1, keepdims=True))
    return centered * lax.rsqrt(variance + NORM_EPS) * gain_vector + shift_vector

def split_vector(vector):
    pieces = [vector[index * D:(index + 1) * D] for index in range(8)]
    return tuple(pieces) + (vector[8 * D:8 * D + FF],)

def tiled(stack, count_rows, count_cols):
    block_side = stack.shape[-1]
    return stack.reshape(count_rows, count_cols, block_side, block_side).transpose(0, 2, 1, 3).reshape(count_rows * block_side, count_cols * block_side)

def untiled(matrix, block_side):
    count_rows = matrix.shape[0] // block_side
    count_cols = matrix.shape[1] // block_side
    return matrix.reshape(count_rows, block_side, count_cols, block_side).transpose(0, 2, 1, 3).reshape(count_rows * count_cols, block_side, block_side)

def assemble(blocks):
    block_side = blocks.shape[-1]
    row_tiles = D // block_side
    wide_tiles = FF // block_side
    square = row_tiles * row_tiles
    wide_count = row_tiles * wide_tiles
    mats = [tiled(blocks[index * square:(index + 1) * square], row_tiles, row_tiles) for index in range(4)]
    mats.append(tiled(blocks[4 * square:4 * square + wide_count], row_tiles, wide_tiles))
    mats.append(tiled(blocks[4 * square + wide_count:4 * square + 2 * wide_count], wide_tiles, row_tiles))
    return tuple(mats)

def disassemble(mats, block_side):
    return jnp.concatenate([untiled(matrix, block_side) for matrix in mats], axis=0)

def soap_update(gradient, weight, moment_one, moment_two, left_basis, right_basis):
    rotated = jnp.matmul(jnp.matmul(jnp.swapaxes(left_basis, -1, -2), gradient, precision=HIGHEST), right_basis, precision=HIGHEST)
    moment_one = BETA_ONE * moment_one + (1.0 - BETA_ONE) * rotated
    moment_two = BETA_TWO * moment_two + (1.0 - BETA_TWO) * rotated * rotated
    direction = moment_one / (1.0 - BETA_ONE ** STEP) / (jnp.sqrt(moment_two / (1.0 - BETA_TWO ** STEP)) + ADAM_EPS)
    restored = jnp.matmul(jnp.matmul(left_basis, direction, precision=HIGHEST), jnp.swapaxes(right_basis, -1, -2), precision=HIGHEST)
    return (weight - LR_MATRIX * (restored + DECAY_RATE * weight), moment_one, moment_two)

def adam_update(gradient, weight, moment_one, moment_two):
    moment_one = BETA_ONE * moment_one + (1.0 - BETA_ONE) * gradient
    moment_two = BETA_TWO * moment_two + (1.0 - BETA_TWO) * gradient * gradient
    direction = moment_one / (1.0 - BETA_ONE ** STEP) / (jnp.sqrt(moment_two / (1.0 - BETA_TWO ** STEP)) + ADAM_EPS)
    return (weight - LR_VECTOR * direction, moment_one, moment_two)

def forward(mats, vector, inputs, cotangent, segment_id, span_starts, pairing):
    w_query, w_key, w_value, w_output, w_inner, w_outer = mats
    gain_one, shift_one, gain_two, shift_two, bias_query, bias_value, bias_output, bias_outer, bias_inner = split_vector(vector)
    lead_shape = inputs.shape[:3]
    heads_shape = lead_shape + (HEADS, HEAD_DIM)
    flat_input = inputs.reshape(-1, D)
    queries = low(low_back(product(flat_input, w_query) + bias_query)).reshape(heads_shape)
    key_heads = low(low_back(product(flat_input, w_key))).reshape(heads_shape)
    value_heads = low(low_back(product(flat_input, w_value) + bias_value)).reshape(heads_shape)
    logits = low_back(jnp.einsum('pqihd,pqjhd->pqhij', queries, key_heads, precision=HIGHEST))
    allowed = segment_id[..., :, None] == segment_id[..., None, :]
    scores = jnp.where(allowed[:, :, None], logits * (1.0 / math.sqrt(HEAD_DIM)), -1e+30)
    attn_probs = low(jax.nn.softmax(scores, axis=-1))
    mixed_heads = jnp.einsum('pqhij,pqjhd->pqihd', attn_probs, value_heads, precision=HIGHEST).reshape(-1, D)
    mixed_heads = low(low_back(mixed_heads))
    branch = low_back(product(mixed_heads, w_output) + bias_output)
    normed = layer_norm(flat_input + branch, gain_one, shift_one)
    inner_sum = low_back(product(low(normed), w_inner) + bias_inner)
    active = low(jax.nn.gelu(inner_sum, approximate=False))
    outer_sum = low_back(product(active, w_outer) + bias_outer)
    result = layer_norm(normed + outer_sum, gain_two, shift_two).reshape(lead_shape + (D,))
    valid_mask = (segment_id < SEGS).astype(jnp.float32)
    objective = jnp.sum(cotangent * result * valid_mask[..., None])
    leaders = jnp.take_along_axis(result, span_starts[..., None], axis=2).reshape(N_PAIR, NSEG, D)
    sent_keys = low(low_back(leaders))
    partner = sent_keys[::-1]
    pair_logits = jnp.einsum('psd,ptd->pst', leaders, partner, precision=HIGHEST) * CLS_SCALE
    totals = jax.nn.logsumexp(pair_logits, axis=-1)
    chosen = jnp.take_along_axis(pair_logits, pairing[..., None], axis=-1)[..., 0]
    objective = objective + CLS_WEIGHT * jnp.sum(totals - chosen)
    return (objective, result)

def reference(inputs, cotangent, span_lengths, pad_lengths, pairing, owner_slot, master, first_moment, second_moment, left_basis, right_basis, vector_master, vector_first, vector_second):
    block_side = master.shape[-1]
    mats = assemble(jnp.take(low(master), owner_slot, axis=0))
    span_ends = jnp.cumsum(span_lengths, axis=-1).astype(jnp.int32)
    span_starts = (span_ends - span_lengths).astype(jnp.int32)
    positions = jnp.arange(LEN, dtype=jnp.int32)
    inside = lax.optimization_barrier(jnp.sum((positions[:, None] >= span_ends[..., None, :-1]).astype(jnp.int32), axis=-1)).astype(jnp.int32)
    segment_id = jnp.where(positions >= LEN - pad_lengths[..., None], SEGS, inside).astype(jnp.int32)

    def regroup(array):
        return jnp.swapaxes(array.reshape((N_PAIR, N_DP, ROWS_DEV) + array.shape[2:]), 0, 1)
    records = (regroup(inputs.astype(jnp.float32)), regroup(cotangent.astype(jnp.float32)), regroup(segment_id), regroup(span_starts), jnp.swapaxes(pairing, 0, 1))
    start_mats = tuple((jnp.zeros_like(matrix) for matrix in mats))
    start_vector = jnp.zeros_like(vector_master)

    def accumulate(running, record):
        group_inputs, group_cot, group_ids, group_starts, group_pairing = record

        def objective_fn(mats_in, vector_in, inputs_in):
            return forward(mats_in, vector_in, inputs_in, group_cot, group_ids, group_starts, group_pairing)
        objective, pullback, result = jax.vjp(objective_fn, mats, vector_master, group_inputs, has_aux=True)
        grad_mats, grad_vector, grad_inputs = pullback(jnp.ones((), jnp.float32))
        running_mats = tuple((first + second for first, second in zip(running[0], grad_mats)))
        return ((running_mats, running[1] + grad_vector), (result.astype(jnp.bfloat16), grad_inputs))
    (sum_mats, sum_vector), (results, grads) = lax.scan(accumulate, (start_mats, start_vector), records)

    def ungroup(array):
        swapped = jnp.swapaxes(array, 0, 1)
        return swapped.reshape((N_PAIR, N_DP * ROWS_DEV) + swapped.shape[3:])
    grad_scale = 1.0 / (N_PAIR * N_DP)
    grad_blocks = disassemble(sum_mats, block_side) * grad_scale
    weight_grad = jnp.zeros_like(master).at[owner_slot].set(grad_blocks)
    new_master, new_first, new_second = soap_update(weight_grad, master, first_moment, second_moment, left_basis, right_basis)
    vector_grad = sum_vector * grad_scale
    new_vector, vector_one, vector_two = adam_update(vector_grad, vector_master, vector_first, vector_second)
    return (ungroup(results), ungroup(grads), weight_grad, new_master, new_first, new_second, vector_grad, jnp.stack([new_vector, vector_one, vector_two], axis=0))
```

```python
import functools
import math

import jax
import jax.numpy as jnp
from jax import lax
from jax.experimental import pallas as pl
from jax.experimental.pallas import tpu as pltpu
from jax.sharding import PartitionSpec as P

D = 768
HEADS = 12
FF = 3072
SEGS = 4
STEP = 10


HIGHEST = lax.Precision.HIGHEST
BETA_ONE = 0.9
BETA_TWO = 0.95
ADAM_EPS = 1e-08
LR_MATRIX = 0.1
LR_VECTOR = 1.0
DECAY_RATE = 0.01
NORM_EPS = 1e-12
CLS_SCALE = 0.0625
CLS_WEIGHT = 4.0


def swapped(array, axis, stride):
    return lax.ppermute(array, axis, [(i, i ^ 1 << stride) for i in range(lax.axis_size(axis))])


def layer_norm(values, gain_vector, shift_vector):
    average = jnp.mean(values, axis=-1, keepdims=True)
    centered = values - average
    variance = jnp.mean(centered * centered, axis=-1, keepdims=True)
    return centered * lax.rsqrt(variance + NORM_EPS) * gain_vector + shift_vector


def gelu_exact(values):
    return jax.nn.gelu(values, approximate=False)


def split_vector(vector):
    pieces = [vector[index * D : (index + 1) * D] for index in range(8)]
    return tuple(pieces) + (vector[8 * D : 8 * D + FF],)


def tiled(stack, count_rows, count_cols):
    block_side = stack.shape[-1]
    return (
        stack.reshape(count_rows, count_cols, block_side, block_side)
        .transpose(0, 2, 1, 3)
        .reshape(count_rows * block_side, count_cols * block_side)
    )


def untiled(matrix, block_side):
    count_rows = matrix.shape[0] // block_side
    count_cols = matrix.shape[1] // block_side
    return (
        matrix.reshape(count_rows, block_side, count_cols, block_side)
        .transpose(0, 2, 1, 3)
        .reshape(count_rows * count_cols, block_side, block_side)
    )


def assemble(blocks):
    block_side = blocks.shape[-1]
    row_tiles = D // block_side
    wide_tiles = FF // block_side
    square = row_tiles * row_tiles
    wide_count = row_tiles * wide_tiles
    mats = [
        tiled(blocks[index * square : (index + 1) * square], row_tiles, row_tiles)
        for index in range(4)
    ]
    mats.append(tiled(blocks[4 * square : 4 * square + wide_count], row_tiles, wide_tiles))
    mats.append(
        tiled(blocks[4 * square + wide_count : 4 * square + 2 * wide_count], wide_tiles, row_tiles)
    )
    return tuple(mats)


def disassemble(mats, block_side):
    return jnp.concatenate([untiled(matrix, block_side) for matrix in mats], axis=0)


def soap_update(gradient, weight, moment_one, moment_two, left_basis, right_basis):
    rotated = jnp.matmul(
        jnp.matmul(jnp.swapaxes(left_basis, -1, -2), gradient, precision=HIGHEST),
        right_basis,
        precision=HIGHEST,
    )
    moment_one = BETA_ONE * moment_one + (1.0 - BETA_ONE) * rotated
    moment_two = BETA_TWO * moment_two + (1.0 - BETA_TWO) * rotated * rotated
    direction = (
        moment_one
        / (1.0 - BETA_ONE**STEP)
        / (jnp.sqrt(moment_two / (1.0 - BETA_TWO**STEP)) + ADAM_EPS)
    )
    restored = jnp.matmul(
        jnp.matmul(left_basis, direction, precision=HIGHEST),
        jnp.swapaxes(right_basis, -1, -2),
        precision=HIGHEST,
    )
    return (weight - LR_MATRIX * (restored + DECAY_RATE * weight), moment_one, moment_two)


def adam_update(gradient, weight, moment_one, moment_two):
    moment_one = BETA_ONE * moment_one + (1.0 - BETA_ONE) * gradient
    moment_two = BETA_TWO * moment_two + (1.0 - BETA_TWO) * gradient * gradient
    direction = (
        moment_one
        / (1.0 - BETA_ONE**STEP)
        / (jnp.sqrt(moment_two / (1.0 - BETA_TWO**STEP)) + ADAM_EPS)
    )
    return (weight - LR_VECTOR * direction, moment_one, moment_two)


def scores_of(left, right):
    return lax.dot_general(
        left, right, (((1,), (1,)), ((), ())), preferred_element_type=jnp.float32
    )


def attend_forward_body(head_dim, seg_col, seg_row, q_ref, k_ref, v_ref, o_ref):
    allowed = seg_col[0] == seg_row[0]
    factor = 1.0 / math.sqrt(head_dim)
    for start in range(0, q_ref.shape[1], head_dim):
        lanes = slice(start, start + head_dim)
        scores = scores_of(q_ref[:, lanes], k_ref[:, lanes])
        scores = jnp.where(allowed, scores * factor, -1e30)
        top = jnp.max(scores, axis=1, keepdims=True)
        weights = jnp.exp(scores - top)
        total = jnp.sum(weights, axis=1, keepdims=True)
        probs = (weights * (1.0 / total)).astype(jnp.bfloat16)
        mixed = jnp.dot(probs, v_ref[:, lanes], preferred_element_type=jnp.float32)
        o_ref[:, lanes] = mixed.astype(o_ref.dtype)


def attend_backward_body(
    head_dim, seg_col, seg_row, q_ref, k_ref, v_ref, g_ref, dq_ref, dk_ref, dv_ref
):
    allowed = seg_col[0] == seg_row[0]
    factor = 1.0 / math.sqrt(head_dim)
    for start in range(0, q_ref.shape[1], head_dim):
        lanes = slice(start, start + head_dim)
        query, key = q_ref[:, lanes], k_ref[:, lanes]
        value, grad = v_ref[:, lanes], g_ref[:, lanes]
        scores = jnp.where(allowed, scores_of(key, query) * factor, -1e30)
        top = jnp.max(scores, axis=0, keepdims=True)
        weights = jnp.exp(scores - top)
        total = jnp.sum(weights, axis=0, keepdims=True)
        probs = weights * (1.0 / total)
        dv = jnp.dot(probs.astype(jnp.bfloat16), grad, preferred_element_type=jnp.float32)
        dv_ref[:, lanes] = dv.astype(dv_ref.dtype)
        grad_probs = scores_of(value, grad)
        inner = jnp.sum(probs * grad_probs, axis=0, keepdims=True)
        grad_scores = probs * (grad_probs - inner)
        grad_logits = jnp.where(allowed, grad_scores * factor, 0.0).astype(jnp.bfloat16)
        dk = jnp.dot(grad_logits, query, preferred_element_type=jnp.float32)
        dk_ref[:, lanes] = dk.astype(dk_ref.dtype)
        dq = lax.dot_general(
            grad_logits, key, (((0,), (0,)), ((), ())), preferred_element_type=jnp.float32
        )
        dq_ref[:, lanes] = dq.astype(dq_ref.dtype)


def attention_call(body, count_out, segment_id, arrays):
    rows, seq_len = segment_id.shape
    width = arrays[0].shape[1]
    lanes = 2 * (D // HEADS)
    tile = pl.BlockSpec((seq_len, lanes), lambda r, h: (r, h))
    shape = jax.ShapeDtypeStruct(arrays[0].shape, jnp.bfloat16)
    flops = 2 * rows * seq_len * seq_len * width * (2 if count_out == 1 else 5)
    return pl.pallas_call(
        functools.partial(body, D // HEADS),
        grid=(rows, width // lanes),
        in_specs=[
            pl.BlockSpec((1, seq_len, 1), lambda r, h: (r, 0, 0)),
            pl.BlockSpec((1, 1, seq_len), lambda r, h: (r, 0, 0)),
        ]
        + [tile] * len(arrays),
        out_specs=[tile] * count_out,
        out_shape=[shape] * count_out,
        cost_estimate=pl.CostEstimate(
            flops=flops,
            bytes_accessed=2 * arrays[0].size * (len(arrays) + count_out),
            transcendentals=rows * HEADS * seq_len * seq_len,
        ),
    )(segment_id[:, :, None], segment_id[:, None, :], *arrays)


def per_device(
    inputs,
    cotangent,
    span_lengths,
    pad_lengths,
    pairing,
    owner_slot,
    master,
    first_moment,
    second_moment,
    left_basis,
    right_basis,
    vector_master,
    vector_first,
    vector_second,
):
    pair_count = lax.axis_size("pair")
    data_count = lax.axis_size("dp")
    grad_scale = 1.0 / (pair_count * data_count)
    block_side = master.shape[-1]
    half = block_side // pair_count
    core = lax.axis_index("pair")
    own_half = lax.dynamic_slice_in_dim(master, core * half, half, axis=1).astype(jnp.bfloat16)
    gathered = lax.all_gather(own_half, ("dp", "pair"), axis=0)
    gathered = gathered.reshape(data_count, pair_count, -1, half, block_side)
    gathered = gathered.transpose(0, 2, 1, 3, 4).reshape(-1, block_side, block_side)
    w_query, w_key, w_value, w_output, w_inner, w_outer = assemble(
        gathered.at[owner_slot].get(mode="promise_in_bounds", unique_indices=True)
    )
    (
        gain_one,
        shift_one,
        gain_two,
        shift_two,
        bias_query,
        bias_value,
        bias_output,
        bias_outer,
        bias_inner,
    ) = split_vector(vector_master)
    row_count = inputs.shape[1]
    seq_len = inputs.shape[2]
    token_count = row_count * seq_len
    flat_input = inputs.reshape(token_count, D)
    span_rows = span_lengths[0]
    pad_rows = pad_lengths[0]
    span_ends = jnp.cumsum(span_rows, axis=-1)
    span_starts = span_ends - span_rows
    positions = jnp.arange(seq_len, dtype=jnp.int32)
    inside = jnp.sum(
        (positions[None, :, None] >= span_ends[:, None, :-1]).astype(jnp.int32), axis=-1
    )
    segment_id = jnp.where(positions[None, :] >= seq_len - pad_rows[:, None], SEGS, inside)
    query_rows = (
        (jnp.dot(flat_input, w_query, preferred_element_type=jnp.float32) + bias_query)
        .astype(jnp.bfloat16)
    )
    key_rows = (
        jnp.dot(flat_input, w_key, preferred_element_type=jnp.float32)
        .astype(jnp.bfloat16)
    )
    value_rows = (
        (jnp.dot(flat_input, w_value, preferred_element_type=jnp.float32) + bias_value)
        .astype(jnp.bfloat16)
    )
    (mixed_low,) = attention_call(
        attend_forward_body, 1, segment_id, (query_rows, key_rows, value_rows)
    )
    branch = jnp.dot(mixed_low, w_output, preferred_element_type=jnp.float32) + bias_output
    residual_one = flat_input.astype(jnp.float32) + branch
    normed = layer_norm(residual_one, gain_one, shift_one)
    normed_low = normed.astype(jnp.bfloat16)
    inner_sum = jnp.dot(normed_low, w_inner, preferred_element_type=jnp.float32) + bias_inner
    active_low = gelu_exact(inner_sum).astype(jnp.bfloat16)
    outer_sum = jnp.dot(active_low, w_outer, preferred_element_type=jnp.float32) + bias_outer
    residual_two = normed + outer_sum
    result = layer_norm(residual_two, gain_two, shift_two)
    result_rows = result.reshape(row_count, seq_len, D)
    leaders = jnp.take_along_axis(result_rows, span_starts[:, :, None], axis=1).reshape(-1, D)
    partner = swapped(leaders.astype(jnp.bfloat16), "pair", 0).astype(jnp.float32)
    pair_logits = (
        jnp.dot(leaders, partner.T, precision=HIGHEST, preferred_element_type=jnp.float32)
        * CLS_SCALE
    )
    pair_probs = jax.nn.softmax(pair_logits, axis=-1)
    targets = (
        pairing.reshape(-1)[:, None] == jnp.arange(leaders.shape[0], dtype=jnp.int32)[None, :]
    ).astype(jnp.float32)
    grad_pair = CLS_WEIGHT * CLS_SCALE * (pair_probs - targets)
    grad_leaders = jnp.dot(
        grad_pair, partner, precision=HIGHEST, preferred_element_type=jnp.float32
    )
    grad_partner = jnp.dot(
        grad_pair.T, leaders, precision=HIGHEST, preferred_element_type=jnp.float32
    )
    returned = swapped(grad_partner.astype(jnp.bfloat16), "pair", 0).astype(jnp.float32)
    grad_leaders = grad_leaders + returned
    valid_mask = (segment_id < SEGS).astype(jnp.float32)
    grad_result = cotangent[0].astype(jnp.float32) * valid_mask[:, :, None]
    row_index = jnp.arange(row_count, dtype=jnp.int32)[:, None]
    grad_result = grad_result.at[row_index, span_starts].add(
        grad_leaders.reshape(row_count, SEGS, D)
    )
    grad_result = grad_result.reshape(token_count, D)
    primal_two, norm_two_back = jax.vjp(layer_norm, residual_two, gain_two, shift_two)
    grad_residual_two, grad_gain_two, grad_shift_two = norm_two_back(grad_result)
    grad_outer = grad_residual_two.astype(jnp.bfloat16)
    grad_bias_outer = jnp.sum(grad_outer, axis=0, dtype=jnp.float32)
    grad_w_outer = jnp.einsum(
        "tf,td->fd", active_low, grad_outer, preferred_element_type=jnp.float32
    )
    grad_active = jnp.einsum("td,fd->tf", grad_outer, w_outer, preferred_element_type=jnp.float32)
    primal_gelu, gelu_back = jax.vjp(gelu_exact, inner_sum)
    grad_inner = gelu_back(grad_active)[0].astype(jnp.bfloat16)
    grad_bias_inner = jnp.sum(grad_inner, axis=0, dtype=jnp.float32)
    grad_w_inner = jnp.einsum(
        "td,tf->df", normed_low, grad_inner, preferred_element_type=jnp.float32
    )
    grad_normed = grad_residual_two + jnp.einsum(
        "tf,df->td", grad_inner, w_inner, preferred_element_type=jnp.float32
    )
    primal_one, norm_one_back = jax.vjp(layer_norm, residual_one, gain_one, shift_one)
    grad_residual_one, grad_gain_one, grad_shift_one = norm_one_back(grad_normed)
    grad_branch = grad_residual_one.astype(jnp.bfloat16)
    grad_bias_output = jnp.sum(grad_branch, axis=0, dtype=jnp.float32)
    grad_w_output = jnp.einsum(
        "td,te->de", mixed_low, grad_branch, preferred_element_type=jnp.float32
    )
    grad_mixed = (
        jnp.einsum("te,de->td", grad_branch, w_output, preferred_element_type=jnp.float32)
        .astype(jnp.bfloat16)
    )
    grad_query, grad_key, grad_value = attention_call(
        attend_backward_body, 3, segment_id, (query_rows, key_rows, value_rows, grad_mixed)
    )
    grad_bias_query = jnp.sum(grad_query, axis=0, dtype=jnp.float32)
    grad_bias_value = jnp.sum(grad_value, axis=0, dtype=jnp.float32)
    grad_w_query = jnp.einsum(
        "td,te->de", flat_input, grad_query, preferred_element_type=jnp.float32
    )
    grad_w_key = jnp.einsum("td,te->de", flat_input, grad_key, preferred_element_type=jnp.float32)
    grad_w_value = jnp.einsum(
        "td,te->de", flat_input, grad_value, preferred_element_type=jnp.float32
    )
    grad_inputs = grad_residual_one + jnp.einsum(
        "te,de->td", grad_query, w_query, preferred_element_type=jnp.float32
    )
    grad_inputs = grad_inputs + jnp.einsum(
        "te,de->td", grad_key, w_key, preferred_element_type=jnp.float32
    )
    grad_inputs = grad_inputs + jnp.einsum(
        "te,de->td", grad_value, w_value, preferred_element_type=jnp.float32
    )
    local_vector = (
        jnp.concatenate(
            [
                grad_gain_one,
                grad_shift_one,
                grad_gain_two,
                grad_shift_two,
                grad_bias_query,
                grad_bias_value,
                grad_bias_output,
                grad_bias_outer,
                grad_bias_inner,
            ]
        )
        * grad_scale
    )
    vector_grad = lax.psum(local_vector, ("pair", "dp"))
    grad_blocks = disassemble(
        tuple(
            (matrix * grad_scale).astype(jnp.bfloat16)
            for matrix in (
                grad_w_query, grad_w_key, grad_w_value, grad_w_output, grad_w_inner, grad_w_outer
            )
        ),
        block_side,
    )
    slot_total = master.shape[0] * data_count
    block_of = (
        jnp.full((slot_total,), owner_slot.shape[0], jnp.int32)
        .at[owner_slot]
        .set(jnp.arange(owner_slot.shape[0], dtype=jnp.int32))
    )
    padded = jnp.concatenate(
        [grad_blocks, jnp.zeros((1, block_side, block_side), jnp.bfloat16)], axis=0
    )
    dealt_grad = padded.at[block_of].get(mode="promise_in_bounds")
    own_grad = lax.psum_scatter(dealt_grad, "pair", scatter_dimension=1, tiled=True)
    own_grad = lax.psum_scatter(own_grad, "dp", scatter_dimension=0, tiled=True)
    owned_grad = lax.all_gather(own_grad, "pair", axis=1, tiled=True).astype(jnp.float32)
    new_master, new_first, new_second = soap_update(
        owned_grad, master, first_moment, second_moment, left_basis, right_basis
    )
    new_vector, vector_one, vector_two = adam_update(
        vector_grad, vector_master, vector_first, vector_second
    )
    return (
        result_rows.astype(jnp.bfloat16).reshape(inputs.shape),
        grad_inputs.reshape(inputs.shape),
        owned_grad,
        new_master,
        new_first,
        new_second,
        vector_grad,
        jnp.stack([new_vector, vector_one, vector_two], axis=0),
    )


def solution(mesh):
    placed = (
        P("pair", "dp", None, None),
        P("pair", "dp", None, None),
        P("pair", "dp", None),
        P("pair", "dp"),
        P("pair", "dp", None),
        P(),
        P("dp", None, None),
        P("dp", None, None),
        P("dp", None, None),
        P("dp", None, None),
        P("dp", None, None),
        P(),
        P(),
        P(),
    )
    return jax.shard_map(
        per_device,
        mesh=mesh,
        in_specs=placed,
        out_specs=(
            P("pair", "dp", None, None),
            P("pair", "dp", None, None),
            P("dp", None, None),
            P("dp", None, None),
            P("dp", None, None),
            P("dp", None, None),
            P(),
            P(),
        ),
        check_vma=False,
    )
```

```python
import functools
import math

import jax
import jax.numpy as jnp
from jax import lax
from jax.experimental import pallas as pl
from jax.experimental.pallas import tpu as pltpu
from jax.sharding import PartitionSpec as P

D = 768
HEADS = 12
FF = 3072
SEGS = 4
STEP = 10


HIGHEST = lax.Precision.HIGHEST
BETA_ONE = 0.9
BETA_TWO = 0.95
ADAM_EPS = 1e-08
LR_MATRIX = 0.1
LR_VECTOR = 1.0
DECAY_RATE = 0.01
NORM_EPS = 1e-12
CLS_SCALE = 0.0625
CLS_WEIGHT = 4.0


def swapped(array, axis, stride):
    return lax.ppermute(array, axis, [(i, i ^ 1 << stride) for i in range(lax.axis_size(axis))])


def layer_norm(values, gain_vector, shift_vector):
    average = jnp.mean(values, axis=-1, keepdims=True)
    centered = values - average
    variance = jnp.mean(centered * centered, axis=-1, keepdims=True)
    return centered * lax.rsqrt(variance + NORM_EPS) * gain_vector + shift_vector


def gelu_and_slope(values):
    lower = 0.5 * (1.0 + lax.erf(values * math.sqrt(0.5)))
    density = jnp.exp(-0.5 * values * values) * (1.0 / math.sqrt(2.0 * math.pi))
    return values * lower, lower + values * density


def split_vector(vector):
    pieces = [vector[index * D : (index + 1) * D] for index in range(8)]
    return tuple(pieces) + (vector[8 * D : 8 * D + FF],)


def matrix_shapes():
    return ((D, D),) * 4 + ((D, FF), (FF, D))


def tile_walk(block_side):
    for index, (rows, cols) in enumerate(matrix_shapes()):
        for row in range(rows // block_side):
            for col in range(cols // block_side):
                yield index, row, col


def assemble_body(per_owner, halves, slot_ref, gathered_ref, *refs):
    mats, sems = refs[:-1], refs[-1]
    half, side = gathered_ref.shape[-2:]
    for block, (index, row, col) in enumerate(tile_walk(side)):
        slot = slot_ref[block]
        owner, place = lax.div(slot, per_owner), lax.rem(slot, per_owner)
        for part in range(halves):
            pltpu.make_async_copy(
                gathered_ref.at[owner * halves + part, place],
                mats[index].at[
                    pl.ds(row * side + part * half, half), pl.ds(col * side, side)
                ],
                sems.at[index],
            ).start()
    for index, matrix in enumerate(mats):
        pltpu.make_async_copy(matrix, matrix, sems.at[index]).wait()


def assemble(gathered, owner_slot, halves):
    shapes = matrix_shapes()
    return pl.pallas_call(
        functools.partial(assemble_body, gathered.shape[1], halves),
        in_specs=[
            pl.BlockSpec(memory_space=pltpu.SMEM),
            pl.BlockSpec(memory_space=pl.ANY),
        ],
        out_specs=[pl.BlockSpec(memory_space=pltpu.VMEM)] * len(shapes),
        out_shape=[jax.ShapeDtypeStruct(shape, gathered.dtype) for shape in shapes],
        scratch_shapes=[pltpu.SemaphoreType.DMA((len(shapes),))],
        cost_estimate=pl.CostEstimate(
            flops=0, bytes_accessed=4 * gathered.size, transcendentals=0
        ),
    )(owner_slot, gathered)


def deal_body(side, slot_ref, zero_ref, *refs):
    mats, (dealt_ref, used_ref, sem) = refs[:-3], refs[-3:]
    half = dealt_ref.shape[1]

    @pl.loop(0, dealt_ref.shape[0])
    def _(slot):
        used_ref[slot] = 0

    for block, (index, row, col) in enumerate(tile_walk(side)):
        slot = slot_ref[block]
        used_ref[slot] = 1
        pltpu.make_async_copy(
            mats[index].at[pl.ds(row * half, half), pl.ds(col * side, side)],
            dealt_ref.at[slot],
            sem,
        ).start()

    @pl.loop(0, dealt_ref.shape[0])
    def _(slot):
        @pl.when(used_ref[slot] == 0)
        def _():
            pltpu.make_async_copy(zero_ref, dealt_ref.at[slot], sem).start()

    pltpu.make_async_copy(dealt_ref, dealt_ref, sem).wait()


def deal(mats, owner_slot, slot_total, half, side):
    dtype = mats[0].dtype
    return pl.pallas_call(
        functools.partial(deal_body, side),
        in_specs=[pl.BlockSpec(memory_space=pltpu.SMEM)]
        + [pl.BlockSpec(memory_space=pltpu.VMEM)] * (1 + len(mats)),
        out_specs=pl.BlockSpec(memory_space=pl.ANY),
        out_shape=jax.ShapeDtypeStruct((slot_total, half, side), dtype),
        scratch_shapes=[pltpu.SMEM((slot_total,), jnp.int32), pltpu.SemaphoreType.DMA],
        cost_estimate=pl.CostEstimate(
            flops=0, bytes_accessed=4 * slot_total * half * side, transcendentals=0
        ),
    )(owner_slot, jnp.zeros((half, side), dtype), *mats)


def pair_summed(gradient, scale, block_side, core):
    halves = lax.axis_size("pair")
    half = block_side // halves
    gradient = (gradient * scale).astype(jnp.bfloat16)
    parts = gradient.reshape(-1, halves, half, gradient.shape[1])
    sent = lax.dynamic_index_in_dim(parts, 1 - core, axis=1, keepdims=False)
    kept = lax.dynamic_index_in_dim(parts, core, axis=1, keepdims=False)
    total = kept.astype(jnp.float32) + swapped(sent, "pair", 0).astype(jnp.float32)
    return total.astype(jnp.bfloat16).reshape(-1, gradient.shape[1])


def soap_update(gradient, weight, moment_one, moment_two, left_basis, right_basis):
    rotated = jnp.matmul(
        jnp.matmul(jnp.swapaxes(left_basis, -1, -2), gradient, precision=HIGHEST),
        right_basis,
        precision=HIGHEST,
    )
    moment_one = BETA_ONE * moment_one + (1.0 - BETA_ONE) * rotated
    moment_two = BETA_TWO * moment_two + (1.0 - BETA_TWO) * rotated * rotated
    direction = (
        moment_one
        / (1.0 - BETA_ONE**STEP)
        / (jnp.sqrt(moment_two / (1.0 - BETA_TWO**STEP)) + ADAM_EPS)
    )
    restored = jnp.matmul(
        jnp.matmul(left_basis, direction, precision=HIGHEST),
        jnp.swapaxes(right_basis, -1, -2),
        precision=HIGHEST,
    )
    return (weight - LR_MATRIX * (restored + DECAY_RATE * weight), moment_one, moment_two)


def adam_update(gradient, weight, moment_one, moment_two):
    moment_one = BETA_ONE * moment_one + (1.0 - BETA_ONE) * gradient
    moment_two = BETA_TWO * moment_two + (1.0 - BETA_TWO) * gradient * gradient
    direction = (
        moment_one
        / (1.0 - BETA_ONE**STEP)
        / (jnp.sqrt(moment_two / (1.0 - BETA_TWO**STEP)) + ADAM_EPS)
    )
    return (weight - LR_VECTOR * direction, moment_one, moment_two)


def scores_of(left, right):
    return lax.dot_general(
        left, right, (((1,), (1,)), ((), ())), preferred_element_type=jnp.float32
    )


def attend_forward_body(head_dim, seg_col, seg_row, q_ref, k_ref, v_ref, o_ref):
    allowed = seg_col[0] == seg_row[0]
    factor = 1.0 / math.sqrt(head_dim)
    for start in range(0, q_ref.shape[1], head_dim):
        lanes = slice(start, start + head_dim)
        scores = scores_of(q_ref[:, lanes], k_ref[:, lanes])
        scores = jnp.where(allowed, scores * factor, -1e30)
        top = jnp.max(scores, axis=1, keepdims=True)
        weights = jnp.exp(scores - top)
        total = jnp.sum(weights, axis=1, keepdims=True)
        probs = (weights * (1.0 / total)).astype(jnp.bfloat16)
        mixed = jnp.dot(probs, v_ref[:, lanes], preferred_element_type=jnp.float32)
        o_ref[:, lanes] = mixed.astype(o_ref.dtype)


def attend_backward_body(
    head_dim, seg_col, seg_row, q_ref, k_ref, v_ref, g_ref, dq_ref, dk_ref, dv_ref
):
    allowed = seg_col[0] == seg_row[0]
    factor = 1.0 / math.sqrt(head_dim)
    for start in range(0, q_ref.shape[1], head_dim):
        lanes = slice(start, start + head_dim)
        query, key = q_ref[:, lanes], k_ref[:, lanes]
        value, grad = v_ref[:, lanes], g_ref[:, lanes]
        scores = jnp.where(allowed, scores_of(key, query) * factor, -1e30)
        top = jnp.max(scores, axis=0, keepdims=True)
        weights = jnp.exp(scores - top)
        total = jnp.sum(weights, axis=0, keepdims=True)
        probs = weights * (1.0 / total)
        dv = jnp.dot(probs.astype(jnp.bfloat16), grad, preferred_element_type=jnp.float32)
        dv_ref[:, lanes] = dv.astype(dv_ref.dtype)
        grad_probs = scores_of(value, grad)
        inner = jnp.sum(probs * grad_probs, axis=0, keepdims=True)
        grad_scores = probs * (grad_probs - inner)
        grad_logits = jnp.where(allowed, grad_scores * factor, 0.0).astype(jnp.bfloat16)
        dk = jnp.dot(grad_logits, query, preferred_element_type=jnp.float32)
        dk_ref[:, lanes] = dk.astype(dk_ref.dtype)
        dq = lax.dot_general(
            grad_logits, key, (((0,), (0,)), ((), ())), preferred_element_type=jnp.float32
        )
        dq_ref[:, lanes] = dq.astype(dq_ref.dtype)


def attention_call(body, count_out, segment_id, arrays):
    rows, seq_len = segment_id.shape
    width = arrays[0].shape[1]
    lanes = 2 * (D // HEADS)
    tile = pl.BlockSpec((seq_len, lanes), lambda r, h: (r, h))
    shape = jax.ShapeDtypeStruct(arrays[0].shape, jnp.bfloat16)
    flops = 2 * rows * seq_len * seq_len * width * (2 if count_out == 1 else 5)
    return pl.pallas_call(
        functools.partial(body, D // HEADS),
        grid=(rows, width // lanes),
        in_specs=[
            pl.BlockSpec((1, seq_len, 1), lambda r, h: (r, 0, 0)),
            pl.BlockSpec((1, 1, seq_len), lambda r, h: (r, 0, 0)),
        ]
        + [tile] * len(arrays),
        out_specs=[tile] * count_out,
        out_shape=[shape] * count_out,
        cost_estimate=pl.CostEstimate(
            flops=flops,
            bytes_accessed=2 * arrays[0].size * (len(arrays) + count_out),
            transcendentals=rows * HEADS * seq_len * seq_len,
        ),
    )(segment_id[:, :, None], segment_id[:, None, :], *arrays)


def per_device(
    inputs,
    cotangent,
    span_lengths,
    pad_lengths,
    pairing,
    owner_slot,
    master,
    first_moment,
    second_moment,
    left_basis,
    right_basis,
    vector_master,
    vector_first,
    vector_second,
):
    pair_count = lax.axis_size("pair")
    data_count = lax.axis_size("dp")
    grad_scale = 1.0 / (pair_count * data_count)
    block_side = master.shape[-1]
    half = block_side // pair_count
    core = lax.axis_index("pair")
    own_half = lax.dynamic_slice_in_dim(master, core * half, half, axis=1).astype(jnp.bfloat16)
    gathered = lax.all_gather(own_half, ("dp", "pair"), axis=0)
    w_query, w_key, w_value, w_output, w_inner, w_outer = assemble(
        gathered, owner_slot, pair_count
    )
    (
        gain_one,
        shift_one,
        gain_two,
        shift_two,
        bias_query,
        bias_value,
        bias_output,
        bias_outer,
        bias_inner,
    ) = split_vector(vector_master)
    row_count = inputs.shape[1]
    seq_len = inputs.shape[2]
    token_count = row_count * seq_len
    flat_input = inputs.reshape(token_count, D)
    span_rows = span_lengths[0]
    pad_rows = pad_lengths[0]
    span_ends = jnp.cumsum(span_rows, axis=-1)
    span_starts = span_ends - span_rows
    positions = jnp.arange(seq_len, dtype=jnp.int32)
    inside = jnp.sum(
        (positions[None, :, None] >= span_ends[:, None, :-1]).astype(jnp.int32), axis=-1
    )
    segment_id = jnp.where(positions[None, :] >= seq_len - pad_rows[:, None], SEGS, inside)
    query_rows = (
        (jnp.dot(flat_input, w_query, preferred_element_type=jnp.float32) + bias_query)
        .astype(jnp.bfloat16)
    )
    key_rows = (
        jnp.dot(flat_input, w_key, preferred_element_type=jnp.float32)
        .astype(jnp.bfloat16)
    )
    value_rows = (
        (jnp.dot(flat_input, w_value, preferred_element_type=jnp.float32) + bias_value)
        .astype(jnp.bfloat16)
    )
    (mixed_low,) = attention_call(
        attend_forward_body, 1, segment_id, (query_rows, key_rows, value_rows)
    )
    branch = jnp.dot(mixed_low, w_output, preferred_element_type=jnp.float32) + bias_output
    residual_one = flat_input.astype(jnp.float32) + branch
    normed = layer_norm(residual_one, gain_one, shift_one)
    normed_low = normed.astype(jnp.bfloat16)
    inner_sum = jnp.dot(normed_low, w_inner, preferred_element_type=jnp.float32) + bias_inner
    active, slope = gelu_and_slope(inner_sum)
    active_low, slope_low = active.astype(jnp.bfloat16), slope.astype(jnp.bfloat16)
    outer_sum = jnp.dot(active_low, w_outer, preferred_element_type=jnp.float32) + bias_outer
    residual_two = normed + outer_sum
    result = layer_norm(residual_two, gain_two, shift_two)
    result_rows = result.reshape(row_count, seq_len, D)
    leaders = jnp.take_along_axis(result_rows, span_starts[:, :, None], axis=1).reshape(-1, D)
    partner = swapped(leaders.astype(jnp.bfloat16), "pair", 0).astype(jnp.float32)
    pair_logits = (
        jnp.dot(leaders, partner.T, precision=HIGHEST, preferred_element_type=jnp.float32)
        * CLS_SCALE
    )
    pair_probs = jax.nn.softmax(pair_logits, axis=-1)
    targets = (
        pairing.reshape(-1)[:, None] == jnp.arange(leaders.shape[0], dtype=jnp.int32)[None, :]
    ).astype(jnp.float32)
    grad_pair = CLS_WEIGHT * CLS_SCALE * (pair_probs - targets)
    grad_leaders = jnp.dot(
        grad_pair, partner, precision=HIGHEST, preferred_element_type=jnp.float32
    )
    grad_partner = jnp.dot(
        grad_pair.T, leaders, precision=HIGHEST, preferred_element_type=jnp.float32
    )
    returned = swapped(grad_partner.astype(jnp.bfloat16), "pair", 0).astype(jnp.float32)
    grad_leaders = grad_leaders + returned
    valid_mask = (segment_id < SEGS).astype(jnp.float32)
    grad_result = cotangent[0].astype(jnp.float32) * valid_mask[:, :, None]
    row_index = jnp.arange(row_count, dtype=jnp.int32)[:, None]
    grad_result = grad_result.at[row_index, span_starts].add(
        grad_leaders.reshape(row_count, SEGS, D)
    )
    grad_result = grad_result.reshape(token_count, D)
    primal_two, norm_two_back = jax.vjp(layer_norm, residual_two, gain_two, shift_two)
    grad_residual_two, grad_gain_two, grad_shift_two = norm_two_back(grad_result)
    grad_outer = grad_residual_two.astype(jnp.bfloat16)
    grad_bias_outer = jnp.sum(grad_outer, axis=0, dtype=jnp.float32)
    grad_w_outer = jnp.einsum(
        "tf,td->fd", active_low, grad_outer, preferred_element_type=jnp.float32
    )
    grad_active = jnp.einsum("td,fd->tf", grad_outer, w_outer, preferred_element_type=jnp.float32)
    grad_inner = (grad_active * slope_low.astype(jnp.float32)).astype(jnp.bfloat16)
    grad_bias_inner = jnp.sum(grad_inner, axis=0, dtype=jnp.float32)
    grad_w_inner = jnp.einsum(
        "td,tf->df", normed_low, grad_inner, preferred_element_type=jnp.float32
    )
    grad_normed = grad_residual_two + jnp.einsum(
        "tf,df->td", grad_inner, w_inner, preferred_element_type=jnp.float32
    )
    primal_one, norm_one_back = jax.vjp(layer_norm, residual_one, gain_one, shift_one)
    grad_residual_one, grad_gain_one, grad_shift_one = norm_one_back(grad_normed)
    grad_branch = grad_residual_one.astype(jnp.bfloat16)
    grad_bias_output = jnp.sum(grad_branch, axis=0, dtype=jnp.float32)
    grad_w_output = jnp.einsum(
        "td,te->de", mixed_low, grad_branch, preferred_element_type=jnp.float32
    )
    grad_mixed = (
        jnp.einsum("te,de->td", grad_branch, w_output, preferred_element_type=jnp.float32)
        .astype(jnp.bfloat16)
    )
    grad_query, grad_key, grad_value = attention_call(
        attend_backward_body, 3, segment_id, (query_rows, key_rows, value_rows, grad_mixed)
    )
    grad_bias_query = jnp.sum(grad_query, axis=0, dtype=jnp.float32)
    grad_bias_value = jnp.sum(grad_value, axis=0, dtype=jnp.float32)
    grad_w_query = jnp.einsum(
        "td,te->de", flat_input, grad_query, preferred_element_type=jnp.float32
    )
    grad_w_key = jnp.einsum("td,te->de", flat_input, grad_key, preferred_element_type=jnp.float32)
    grad_w_value = jnp.einsum(
        "td,te->de", flat_input, grad_value, preferred_element_type=jnp.float32
    )
    grad_inputs = grad_residual_one + jnp.einsum(
        "te,de->td", grad_query, w_query, preferred_element_type=jnp.float32
    )
    grad_inputs = grad_inputs + jnp.einsum(
        "te,de->td", grad_key, w_key, preferred_element_type=jnp.float32
    )
    grad_inputs = grad_inputs + jnp.einsum(
        "te,de->td", grad_value, w_value, preferred_element_type=jnp.float32
    )
    local_vector = (
        jnp.concatenate(
            [
                grad_gain_one,
                grad_shift_one,
                grad_gain_two,
                grad_shift_two,
                grad_bias_query,
                grad_bias_value,
                grad_bias_output,
                grad_bias_outer,
                grad_bias_inner,
            ]
        )
        * grad_scale
    )
    vector_grad = lax.psum(local_vector, ("pair", "dp"))
    grad_mats = [
        pair_summed(matrix, grad_scale, block_side, core)
        for matrix in (
            grad_w_query, grad_w_key, grad_w_value, grad_w_output, grad_w_inner, grad_w_outer
        )
    ]
    own_grad = deal(grad_mats, owner_slot, master.shape[0] * data_count, half, block_side)
    own_grad = lax.psum_scatter(own_grad, "dp", scatter_dimension=0, tiled=True)
    owned_grad = lax.all_gather(own_grad, "pair", axis=1, tiled=True).astype(jnp.float32)
    new_master, new_first, new_second = soap_update(
        owned_grad, master, first_moment, second_moment, left_basis, right_basis
    )
    new_vector, vector_one, vector_two = adam_update(
        vector_grad, vector_master, vector_first, vector_second
    )
    return (
        result_rows.astype(jnp.bfloat16).reshape(inputs.shape),
        grad_inputs.reshape(inputs.shape),
        owned_grad,
        new_master,
        new_first,
        new_second,
        vector_grad,
        jnp.stack([new_vector, vector_one, vector_two], axis=0),
    )


def solution(mesh):
    placed = (
        P("pair", "dp", None, None),
        P("pair", "dp", None, None),
        P("pair", "dp", None),
        P("pair", "dp"),
        P("pair", "dp", None),
        P(),
        P("dp", None, None),
        P("dp", None, None),
        P("dp", None, None),
        P("dp", None, None),
        P("dp", None, None),
        P(),
        P(),
        P(),
    )
    return jax.shard_map(
        per_device,
        mesh=mesh,
        in_specs=placed,
        out_specs=(
            P("pair", "dp", None, None),
            P("pair", "dp", None, None),
            P("dp", None, None),
            P("dp", None, None),
            P("dp", None, None),
            P("dp", None, None),
            P(),
            P(),
        ),
        check_vma=False,
    )
```

```python
import functools
import math

import jax
import jax.numpy as jnp
from jax import lax
from jax.experimental import pallas as pl
from jax.experimental.pallas import tpu as pltpu
from jax.sharding import PartitionSpec as P

D = 768
HEADS = 12
FF = 3072
SEGS = 4
STEP = 10


HIGHEST = lax.Precision.HIGHEST
BETA_ONE = 0.9
BETA_TWO = 0.95
ADAM_EPS = 1e-08
LR_MATRIX = 0.1
LR_VECTOR = 1.0
DECAY_RATE = 0.01
NORM_EPS = 1e-12
CLS_SCALE = 0.0625
CLS_WEIGHT = 4.0


def swapped(array, axis, stride):
    return lax.ppermute(array, axis, [(i, i ^ 1 << stride) for i in range(lax.axis_size(axis))])


def layer_norm(values, gain_vector, shift_vector):
    average = jnp.mean(values, axis=-1, keepdims=True)
    centered = values - average
    variance = jnp.mean(centered * centered, axis=-1, keepdims=True)
    return centered * lax.rsqrt(variance + NORM_EPS) * gain_vector + shift_vector


def gelu_and_slope(values):
    lower = 0.5 * (1.0 + lax.erf(values * math.sqrt(0.5)))
    density = jnp.exp(-0.5 * values * values) * (1.0 / math.sqrt(2.0 * math.pi))
    return values * lower, lower + values * density


def split_vector(vector):
    pieces = [vector[index * D : (index + 1) * D] for index in range(8)]
    return tuple(pieces) + (vector[8 * D : 8 * D + FF],)


def matrix_shapes():
    return ((D, D),) * 4 + ((D, FF), (FF, D))


def tile_walk(block_side):
    for index, (rows, cols) in enumerate(matrix_shapes()):
        for row in range(rows // block_side):
            for col in range(cols // block_side):
                yield index, row, col


def assemble_body(per_owner, halves, slot_ref, gathered_ref, *refs):
    mats, sems = refs[:-1], refs[-1]
    half, side = gathered_ref.shape[-2:]
    for block, (index, row, col) in enumerate(tile_walk(side)):
        slot = slot_ref[block]
        owner, place = lax.div(slot, per_owner), lax.rem(slot, per_owner)
        for part in range(halves):
            pltpu.make_async_copy(
                gathered_ref.at[owner * halves + part, place],
                mats[index].at[
                    pl.ds(row * side + part * half, half), pl.ds(col * side, side)
                ],
                sems.at[index],
            ).start()
    for index, matrix in enumerate(mats):
        pltpu.make_async_copy(matrix, matrix, sems.at[index]).wait()


def assemble(gathered, owner_slot, halves):
    shapes = matrix_shapes()
    return pl.pallas_call(
        functools.partial(assemble_body, gathered.shape[1], halves),
        in_specs=[
            pl.BlockSpec(memory_space=pltpu.SMEM),
            pl.BlockSpec(memory_space=pl.ANY),
        ],
        out_specs=[pl.BlockSpec(memory_space=pltpu.VMEM)] * len(shapes),
        out_shape=[jax.ShapeDtypeStruct(shape, gathered.dtype) for shape in shapes],
        scratch_shapes=[pltpu.SemaphoreType.DMA((len(shapes),))],
        cost_estimate=pl.CostEstimate(
            flops=0, bytes_accessed=4 * gathered.size, transcendentals=0
        ),
    )(owner_slot, gathered)


def deal_body(side, slot_ref, zero_ref, *refs):
    mats, (dealt_ref, used_ref, sem) = refs[:-3], refs[-3:]
    half = dealt_ref.shape[1]

    @pl.loop(0, dealt_ref.shape[0])
    def _(slot):
        used_ref[slot] = 0

    for block, (index, row, col) in enumerate(tile_walk(side)):
        slot = slot_ref[block]
        used_ref[slot] = 1
        pltpu.make_async_copy(
            mats[index].at[pl.ds(row * half, half), pl.ds(col * side, side)],
            dealt_ref.at[slot],
            sem,
        ).start()

    @pl.loop(0, dealt_ref.shape[0])
    def _(slot):
        @pl.when(used_ref[slot] == 0)
        def _():
            pltpu.make_async_copy(zero_ref, dealt_ref.at[slot], sem).start()

    pltpu.make_async_copy(dealt_ref, dealt_ref, sem).wait()


def deal(mats, owner_slot, slot_total, half, side):
    dtype = mats[0].dtype
    return pl.pallas_call(
        functools.partial(deal_body, side),
        in_specs=[pl.BlockSpec(memory_space=pltpu.SMEM)]
        + [pl.BlockSpec(memory_space=pltpu.VMEM)] * (1 + len(mats)),
        out_specs=pl.BlockSpec(memory_space=pl.ANY),
        out_shape=jax.ShapeDtypeStruct((slot_total, half, side), dtype),
        scratch_shapes=[pltpu.SMEM((slot_total,), jnp.int32), pltpu.SemaphoreType.DMA],
        cost_estimate=pl.CostEstimate(
            flops=0, bytes_accessed=4 * slot_total * half * side, transcendentals=0
        ),
    )(owner_slot, jnp.zeros((half, side), dtype), *mats)


MESH_IDS = pl.DeviceIdType.MESH


def spread_body(own_ref, out_ref, send_sem, recv_sem, local_sem):
    core, me = lax.axis_index("pair"), lax.axis_index("dp")
    level, rest = lax.div(me, 4), lax.rem(me, 4)
    flip_y = me + 2 - 4 * lax.div(rest, 2)
    flip_x = me + 1 - 2 * lax.rem(rest, 2)
    first = (1 - core) * flip_y + core * flip_x
    second = (1 - core) * flip_x + core * flip_y
    both = flip_x + flip_y - me
    targets = (
        (core, me + 4), (core, me - 4), (core, first), (core, second), (1 - core, me)
    )

    barrier = pltpu.get_barrier_semaphore()

    def greet(kind):
        pl.semaphore_signal(barrier, inc=1, device_id=targets[kind], device_id_type=MESH_IDS)

    @pl.when(level < 3)
    def _():
        greet(0)

    @pl.when(level > 0)
    def _():
        greet(1)

    for kind in (2, 3, 4):
        greet(kind)

    pl.semaphore_wait(barrier, 3 + lax.div(level + 3, 4) + lax.div(6 - level, 4))

    def link(kind, source, piece=None):
        place = source * 2 + core
        return pltpu.make_async_remote_copy(
            src_ref=out_ref.at[place] if piece is None else piece,
            dst_ref=out_ref.at[place],
            send_sem=send_sem.at[kind, source],
            recv_sem=recv_sem.at[kind // 4, source],
            device_id=targets[kind],
            device_id_type=MESH_IDS,
        )

    def walk(act):
        def line(base, step, kinds, up=(), down=()):
            @pl.when(level >= step)
            def _():
                act(base - 4 * step, kinds, up)

            @pl.when(level + step <= 3)
            def _():
                act(base + 4 * step, kinds, down)

        line(me, 1, (3, 2, 4), (0,), (1,))
        act(first, (3, 4), ())
        line(me, 2, (3, 2, 4), (0,), (1,))
        line(first, 1, (3, 4))
        line(me, 3, (3, 2, 4), (0,), (1,))
        line(first, 2, (3, 4))
        line(first, 3, (3, 4))
        act(second, (4,), ())
        line(second, 1, (4,))
        act(both, (4,), ())
        line(second, 2, (4,))
        line(both, 1, (4,))
        line(second, 3, (4,))
        line(both, 2, (4,))
        line(both, 3, (4,))

    def guarded(kind, run):
        if kind == 0:
            pl.when(level < 3)(run)
        elif kind == 1:
            pl.when(level > 0)(run)
        else:
            run()

    def go(source, kinds, further):
        link(0, source).wait_recv()
        for kind in further + kinds:
            guarded(kind, lambda kind=kind: link(kind, source).start())

    def drain(source, kinds, further):
        for kind in further + kinds:
            guarded(kind, lambda kind=kind: link(kind, source).wait_send())

    for kind in range(5):
        guarded(kind, lambda kind=kind: link(kind, me, own_ref).start())
    local = pltpu.make_async_copy(own_ref, out_ref.at[me * 2 + core], local_sem)
    local.start()
    walk(go)
    for kind in range(5):
        guarded(kind, lambda kind=kind: link(kind, me, own_ref).wait_send())
    walk(drain)

    @pl.loop(0, 16)
    def _(source):
        pltpu.make_async_remote_copy(
            src_ref=own_ref,
            dst_ref=out_ref.at[source * 2 + 1 - core],
            send_sem=send_sem.at[4, source],
            recv_sem=recv_sem.at[1, source],
            device_id=targets[4],
            device_id_type=MESH_IDS,
        ).wait_recv()

    local.wait()


def spread(own, data_count, pair_count):
    if (data_count, pair_count) != (16, 2):
        return lax.all_gather(own, ("dp", "pair"), axis=0)
    return pl.pallas_call(
        spread_body,
        in_specs=[pl.BlockSpec(memory_space=pl.ANY)],
        out_specs=pl.BlockSpec(memory_space=pl.ANY),
        out_shape=jax.ShapeDtypeStruct((32,) + own.shape, own.dtype),
        scratch_shapes=[
            pltpu.SemaphoreType.DMA((5, 16)),
            pltpu.SemaphoreType.DMA((2, 16)),
            pltpu.SemaphoreType.DMA,
        ],
        compiler_params=pltpu.CompilerParams(collective_id=1, has_side_effects=True),
    )(own)


def vector_body(rounds, part_ref, total_ref, held, landed, send_sem, recv_sem):
    core, me = lax.axis_index("pair"), lax.axis_index("dp")
    partners = [(1 - core, me)]
    for step in range(rounds - 1):
        bit = 2**step
        partners.append((core, me + bit - 2 * bit * lax.rem(lax.div(me, bit), 2)))
    barrier = pltpu.get_barrier_semaphore()
    for partner in partners:
        pl.semaphore_signal(barrier, inc=1, device_id=partner, device_id_type=MESH_IDS)
    pl.semaphore_wait(barrier, rounds)
    for step, partner in enumerate(partners):
        source = part_ref if step == 0 else held.at[step - 1]
        copy = pltpu.make_async_remote_copy(
            src_ref=source,
            dst_ref=landed.at[step],
            send_sem=send_sem.at[step],
            recv_sem=recv_sem.at[step],
            device_id=partner,
            device_id_type=MESH_IDS,
        )
        copy.start()
        copy.wait()
        total = source[...] + landed[step]
        if step < rounds - 1:
            held[step] = total
        else:
            total_ref[...] = total


def vector_total(part, data_count, pair_count):
    rounds = data_count.bit_length()
    if pair_count != 2 or 2 ** (rounds - 1) != data_count:
        return lax.psum(part, ("pair", "dp"))
    shape = (part.shape[0] // 128, 128)
    return pl.pallas_call(
        functools.partial(vector_body, rounds),
        in_specs=[pl.BlockSpec(memory_space=pltpu.VMEM)],
        out_specs=pl.BlockSpec(memory_space=pltpu.VMEM),
        out_shape=jax.ShapeDtypeStruct(shape, part.dtype),
        scratch_shapes=[
            pltpu.VMEM((rounds,) + shape, part.dtype),
            pltpu.VMEM((rounds,) + shape, part.dtype),
            pltpu.SemaphoreType.DMA((rounds,)),
            pltpu.SemaphoreType.DMA((rounds,)),
        ],
        compiler_params=pltpu.CompilerParams(collective_id=0, has_side_effects=True),
        cost_estimate=pl.CostEstimate(
            flops=part.size * rounds, bytes_accessed=8 * part.size * rounds, transcendentals=0
        ),
    )(part.reshape(shape)).reshape(-1)


def pair_summed(gradient, scale, block_side, core):
    halves = lax.axis_size("pair")
    half = block_side // halves
    gradient = (gradient * scale).astype(jnp.bfloat16)
    parts = gradient.reshape(-1, halves, half, gradient.shape[1])
    sent = lax.dynamic_index_in_dim(parts, 1 - core, axis=1, keepdims=False)
    kept = lax.dynamic_index_in_dim(parts, core, axis=1, keepdims=False)
    total = kept.astype(jnp.float32) + swapped(sent, "pair", 0).astype(jnp.float32)
    return total.astype(jnp.bfloat16).reshape(-1, gradient.shape[1])


def soap_update(gradient, weight, moment_one, moment_two, left_basis, right_basis):
    rotated = jnp.matmul(
        jnp.matmul(jnp.swapaxes(left_basis, -1, -2), gradient, precision=HIGHEST),
        right_basis,
        precision=HIGHEST,
    )
    moment_one = BETA_ONE * moment_one + (1.0 - BETA_ONE) * rotated
    moment_two = BETA_TWO * moment_two + (1.0 - BETA_TWO) * rotated * rotated
    direction = (
        moment_one
        / (1.0 - BETA_ONE**STEP)
        / (jnp.sqrt(moment_two / (1.0 - BETA_TWO**STEP)) + ADAM_EPS)
    )
    restored = jnp.matmul(
        jnp.matmul(left_basis, direction, precision=HIGHEST),
        jnp.swapaxes(right_basis, -1, -2),
        precision=HIGHEST,
    )
    return (weight - LR_MATRIX * (restored + DECAY_RATE * weight), moment_one, moment_two)


def adam_update(gradient, weight, moment_one, moment_two):
    moment_one = BETA_ONE * moment_one + (1.0 - BETA_ONE) * gradient
    moment_two = BETA_TWO * moment_two + (1.0 - BETA_TWO) * gradient * gradient
    direction = (
        moment_one
        / (1.0 - BETA_ONE**STEP)
        / (jnp.sqrt(moment_two / (1.0 - BETA_TWO**STEP)) + ADAM_EPS)
    )
    return (weight - LR_VECTOR * direction, moment_one, moment_two)


def scores_of(left, right):
    return lax.dot_general(
        left, right, (((1,), (1,)), ((), ())), preferred_element_type=jnp.float32
    )


def attend_forward_body(head_dim, seg_col, seg_row, q_ref, k_ref, v_ref, o_ref):
    allowed = seg_col[0] == seg_row[0]
    factor = 1.0 / math.sqrt(head_dim)
    for start in range(0, q_ref.shape[1], head_dim):
        lanes = slice(start, start + head_dim)
        scores = scores_of(q_ref[:, lanes], k_ref[:, lanes])
        scores = jnp.where(allowed, scores * factor, -1e30)
        top = jnp.max(scores, axis=1, keepdims=True)
        weights = jnp.exp(scores - top)
        total = jnp.sum(weights, axis=1, keepdims=True)
        probs = (weights * (1.0 / total)).astype(jnp.bfloat16)
        mixed = jnp.dot(probs, v_ref[:, lanes], preferred_element_type=jnp.float32)
        o_ref[:, lanes] = mixed.astype(o_ref.dtype)


def attend_backward_body(
    head_dim, seg_col, seg_row, q_ref, k_ref, v_ref, g_ref, dq_ref, dk_ref, dv_ref
):
    allowed = seg_col[0] == seg_row[0]
    factor = 1.0 / math.sqrt(head_dim)
    for start in range(0, q_ref.shape[1], head_dim):
        lanes = slice(start, start + head_dim)
        query, key = q_ref[:, lanes], k_ref[:, lanes]
        value, grad = v_ref[:, lanes], g_ref[:, lanes]
        scores = jnp.where(allowed, scores_of(key, query) * factor, -1e30)
        top = jnp.max(scores, axis=0, keepdims=True)
        weights = jnp.exp(scores - top)
        total = jnp.sum(weights, axis=0, keepdims=True)
        probs = weights * (1.0 / total)
        dv = jnp.dot(probs.astype(jnp.bfloat16), grad, preferred_element_type=jnp.float32)
        dv_ref[:, lanes] = dv.astype(dv_ref.dtype)
        grad_probs = scores_of(value, grad)
        inner = jnp.sum(probs * grad_probs, axis=0, keepdims=True)
        grad_scores = probs * (grad_probs - inner)
        grad_logits = jnp.where(allowed, grad_scores * factor, 0.0).astype(jnp.bfloat16)
        dk = jnp.dot(grad_logits, query, preferred_element_type=jnp.float32)
        dk_ref[:, lanes] = dk.astype(dk_ref.dtype)
        dq = lax.dot_general(
            grad_logits, key, (((0,), (0,)), ((), ())), preferred_element_type=jnp.float32
        )
        dq_ref[:, lanes] = dq.astype(dq_ref.dtype)


def attention_call(body, count_out, segment_id, arrays):
    rows, seq_len = segment_id.shape
    width = arrays[0].shape[1]
    lanes = 2 * (D // HEADS)
    tile = pl.BlockSpec((seq_len, lanes), lambda r, h: (r, h))
    shape = jax.ShapeDtypeStruct(arrays[0].shape, jnp.bfloat16)
    flops = 2 * rows * seq_len * seq_len * width * (2 if count_out == 1 else 5)
    return pl.pallas_call(
        functools.partial(body, D // HEADS),
        grid=(rows, width // lanes),
        in_specs=[
            pl.BlockSpec((1, seq_len, 1), lambda r, h: (r, 0, 0)),
            pl.BlockSpec((1, 1, seq_len), lambda r, h: (r, 0, 0)),
        ]
        + [tile] * len(arrays),
        out_specs=[tile] * count_out,
        out_shape=[shape] * count_out,
        cost_estimate=pl.CostEstimate(
            flops=flops,
            bytes_accessed=2 * arrays[0].size * (len(arrays) + count_out),
            transcendentals=rows * HEADS * seq_len * seq_len,
        ),
    )(segment_id[:, :, None], segment_id[:, None, :], *arrays)


def per_device(
    inputs,
    cotangent,
    span_lengths,
    pad_lengths,
    pairing,
    owner_slot,
    master,
    first_moment,
    second_moment,
    left_basis,
    right_basis,
    vector_master,
    vector_first,
    vector_second,
):
    pair_count = lax.axis_size("pair")
    data_count = lax.axis_size("dp")
    grad_scale = 1.0 / (pair_count * data_count)
    block_side = master.shape[-1]
    half = block_side // pair_count
    core = lax.axis_index("pair")
    own_half = lax.dynamic_slice_in_dim(master, core * half, half, axis=1).astype(jnp.bfloat16)
    gathered = spread(own_half, data_count, pair_count)
    w_query, w_key, w_value, w_output, w_inner, w_outer = assemble(
        gathered, owner_slot, pair_count
    )
    (
        gain_one,
        shift_one,
        gain_two,
        shift_two,
        bias_query,
        bias_value,
        bias_output,
        bias_outer,
        bias_inner,
    ) = split_vector(vector_master)
    row_count = inputs.shape[1]
    seq_len = inputs.shape[2]
    token_count = row_count * seq_len
    flat_input = inputs.reshape(token_count, D)
    span_rows = span_lengths[0]
    pad_rows = pad_lengths[0]
    span_ends = jnp.cumsum(span_rows, axis=-1)
    span_starts = span_ends - span_rows
    positions = jnp.arange(seq_len, dtype=jnp.int32)
    inside = jnp.sum(
        (positions[None, :, None] >= span_ends[:, None, :-1]).astype(jnp.int32), axis=-1
    )
    segment_id = jnp.where(positions[None, :] >= seq_len - pad_rows[:, None], SEGS, inside)
    query_rows = (
        (jnp.dot(flat_input, w_query, preferred_element_type=jnp.float32) + bias_query)
        .astype(jnp.bfloat16)
    )
    key_rows = (
        jnp.dot(flat_input, w_key, preferred_element_type=jnp.float32)
        .astype(jnp.bfloat16)
    )
    value_rows = (
        (jnp.dot(flat_input, w_value, preferred_element_type=jnp.float32) + bias_value)
        .astype(jnp.bfloat16)
    )
    (mixed_low,) = attention_call(
        attend_forward_body, 1, segment_id, (query_rows, key_rows, value_rows)
    )
    branch = jnp.dot(mixed_low, w_output, preferred_element_type=jnp.float32) + bias_output
    residual_one = flat_input.astype(jnp.float32) + branch
    normed = layer_norm(residual_one, gain_one, shift_one)
    normed_low = normed.astype(jnp.bfloat16)
    inner_sum = jnp.dot(normed_low, w_inner, preferred_element_type=jnp.float32) + bias_inner
    active, slope = gelu_and_slope(inner_sum)
    active_low, slope_low = active.astype(jnp.bfloat16), slope.astype(jnp.bfloat16)
    outer_sum = jnp.dot(active_low, w_outer, preferred_element_type=jnp.float32) + bias_outer
    residual_two = normed + outer_sum
    result = layer_norm(residual_two, gain_two, shift_two)
    result_rows = result.reshape(row_count, seq_len, D)
    leaders = jnp.take_along_axis(result_rows, span_starts[:, :, None], axis=1).reshape(-1, D)
    partner = swapped(leaders.astype(jnp.bfloat16), "pair", 0).astype(jnp.float32)
    pair_logits = (
        jnp.dot(leaders, partner.T, precision=HIGHEST, preferred_element_type=jnp.float32)
        * CLS_SCALE
    )
    pair_probs = jax.nn.softmax(pair_logits, axis=-1)
    targets = (
        pairing.reshape(-1)[:, None] == jnp.arange(leaders.shape[0], dtype=jnp.int32)[None, :]
    ).astype(jnp.float32)
    grad_pair = CLS_WEIGHT * CLS_SCALE * (pair_probs - targets)
    grad_leaders = jnp.dot(
        grad_pair, partner, precision=HIGHEST, preferred_element_type=jnp.float32
    )
    grad_partner = jnp.dot(
        grad_pair.T, leaders, precision=HIGHEST, preferred_element_type=jnp.float32
    )
    returned = swapped(grad_partner.astype(jnp.bfloat16), "pair", 0).astype(jnp.float32)
    grad_leaders = grad_leaders + returned
    valid_mask = (segment_id < SEGS).astype(jnp.float32)
    grad_result = cotangent[0].astype(jnp.float32) * valid_mask[:, :, None]
    row_index = jnp.arange(row_count, dtype=jnp.int32)[:, None]
    grad_result = grad_result.at[row_index, span_starts].add(
        grad_leaders.reshape(row_count, SEGS, D)
    )
    grad_result = grad_result.reshape(token_count, D)
    primal_two, norm_two_back = jax.vjp(layer_norm, residual_two, gain_two, shift_two)
    grad_residual_two, grad_gain_two, grad_shift_two = norm_two_back(grad_result)
    grad_outer = grad_residual_two.astype(jnp.bfloat16)
    grad_bias_outer = jnp.sum(grad_outer, axis=0, dtype=jnp.float32)
    grad_w_outer = jnp.einsum(
        "tf,td->fd", active_low, grad_outer, preferred_element_type=jnp.float32
    )
    grad_active = jnp.einsum("td,fd->tf", grad_outer, w_outer, preferred_element_type=jnp.float32)
    grad_inner = (grad_active * slope_low.astype(jnp.float32)).astype(jnp.bfloat16)
    grad_bias_inner = jnp.sum(grad_inner, axis=0, dtype=jnp.float32)
    grad_w_inner = jnp.einsum(
        "td,tf->df", normed_low, grad_inner, preferred_element_type=jnp.float32
    )
    grad_normed = grad_residual_two + jnp.einsum(
        "tf,df->td", grad_inner, w_inner, preferred_element_type=jnp.float32
    )
    primal_one, norm_one_back = jax.vjp(layer_norm, residual_one, gain_one, shift_one)
    grad_residual_one, grad_gain_one, grad_shift_one = norm_one_back(grad_normed)
    grad_branch = grad_residual_one.astype(jnp.bfloat16)
    grad_bias_output = jnp.sum(grad_branch, axis=0, dtype=jnp.float32)
    grad_w_output = jnp.einsum(
        "td,te->de", mixed_low, grad_branch, preferred_element_type=jnp.float32
    )
    grad_mixed = (
        jnp.einsum("te,de->td", grad_branch, w_output, preferred_element_type=jnp.float32)
        .astype(jnp.bfloat16)
    )
    grad_query, grad_key, grad_value = attention_call(
        attend_backward_body, 3, segment_id, (query_rows, key_rows, value_rows, grad_mixed)
    )
    grad_bias_query = jnp.sum(grad_query, axis=0, dtype=jnp.float32)
    grad_bias_value = jnp.sum(grad_value, axis=0, dtype=jnp.float32)
    grad_w_query = jnp.einsum(
        "td,te->de", flat_input, grad_query, preferred_element_type=jnp.float32
    )
    grad_w_key = jnp.einsum("td,te->de", flat_input, grad_key, preferred_element_type=jnp.float32)
    grad_w_value = jnp.einsum(
        "td,te->de", flat_input, grad_value, preferred_element_type=jnp.float32
    )
    grad_inputs = grad_residual_one + jnp.einsum(
        "te,de->td", grad_query, w_query, preferred_element_type=jnp.float32
    )
    grad_inputs = grad_inputs + jnp.einsum(
        "te,de->td", grad_key, w_key, preferred_element_type=jnp.float32
    )
    grad_inputs = grad_inputs + jnp.einsum(
        "te,de->td", grad_value, w_value, preferred_element_type=jnp.float32
    )
    local_vector = (
        jnp.concatenate(
            [
                grad_gain_one,
                grad_shift_one,
                grad_gain_two,
                grad_shift_two,
                grad_bias_query,
                grad_bias_value,
                grad_bias_output,
                grad_bias_outer,
                grad_bias_inner,
            ]
        )
        * grad_scale
    )
    grad_mats = [
        pair_summed(matrix, grad_scale, block_side, core)
        for matrix in (
            grad_w_query, grad_w_key, grad_w_value, grad_w_output, grad_w_inner, grad_w_outer
        )
    ]
    own_grad = deal(grad_mats, owner_slot, master.shape[0] * data_count, half, block_side)
    own_grad, local_vector = lax.optimization_barrier((own_grad, local_vector))
    vector_grad = vector_total(local_vector, data_count, pair_count)
    own_grad = lax.psum_scatter(own_grad, "dp", scatter_dimension=0, tiled=True)
    owned_grad = lax.all_gather(own_grad, "pair", axis=1, tiled=True).astype(jnp.float32)
    new_master, new_first, new_second = soap_update(
        owned_grad, master, first_moment, second_moment, left_basis, right_basis
    )
    new_vector, vector_one, vector_two = adam_update(
        vector_grad, vector_master, vector_first, vector_second
    )
    return (
        result_rows.astype(jnp.bfloat16).reshape(inputs.shape),
        grad_inputs.reshape(inputs.shape),
        owned_grad,
        new_master,
        new_first,
        new_second,
        vector_grad,
        jnp.stack([new_vector, vector_one, vector_two], axis=0),
    )


def solution(mesh):
    placed = (
        P("pair", "dp", None, None),
        P("pair", "dp", None, None),
        P("pair", "dp", None),
        P("pair", "dp"),
        P("pair", "dp", None),
        P(),
        P("dp", None, None),
        P("dp", None, None),
        P("dp", None, None),
        P("dp", None, None),
        P("dp", None, None),
        P(),
        P(),
        P(),
    )
    return jax.shard_map(
        per_device,
        mesh=mesh,
        in_specs=placed,
        out_specs=(
            P("pair", "dp", None, None),
            P("pair", "dp", None, None),
            P("dp", None, None),
            P("dp", None, None),
            P("dp", None, None),
            P("dp", None, None),
            P(),
            P(),
        ),
        check_vma=False,
    )
```

```python
import functools
import math

import jax
import jax.numpy as jnp
from jax import lax
from jax.experimental import pallas as pl
from jax.experimental.pallas import tpu as pltpu
from jax.sharding import PartitionSpec as P

D = 768
HEADS = 12
FF = 3072
SEGS = 4
STEP = 10


HIGHEST = lax.Precision.HIGHEST
BETA_ONE = 0.9
BETA_TWO = 0.95
ADAM_EPS = 1e-08
LR_MATRIX = 0.1
LR_VECTOR = 1.0
DECAY_RATE = 0.01
NORM_EPS = 1e-12
CLS_SCALE = 0.0625
CLS_WEIGHT = 4.0


def swapped(array, axis, stride):
    return lax.ppermute(array, axis, [(i, i ^ 1 << stride) for i in range(lax.axis_size(axis))])


def layer_norm(values, gain_vector, shift_vector):
    average = jnp.mean(values, axis=-1, keepdims=True)
    centered = values - average
    variance = jnp.mean(centered * centered, axis=-1, keepdims=True)
    return centered * lax.rsqrt(variance + NORM_EPS) * gain_vector + shift_vector


def gelu_and_slope(values):
    lower = 0.5 * (1.0 + lax.erf(values * math.sqrt(0.5)))
    density = jnp.exp(-0.5 * values * values) * (1.0 / math.sqrt(2.0 * math.pi))
    return values * lower, lower + values * density


def split_vector(vector):
    pieces = [vector[index * D : (index + 1) * D] for index in range(8)]
    return tuple(pieces) + (vector[8 * D : 8 * D + FF],)


def matrix_shapes():
    return ((D, D),) * 4 + ((D, FF), (FF, D))


def tile_walk(block_side):
    for index, (rows, cols) in enumerate(matrix_shapes()):
        for row in range(rows // block_side):
            for col in range(cols // block_side):
                yield index, row, col


def assemble_body(per_owner, halves, slot_ref, gathered_ref, *refs):
    mats, sems = refs[:-1], refs[-1]
    half, side = gathered_ref.shape[-2:]
    for block, (index, row, col) in enumerate(tile_walk(side)):
        slot = slot_ref[block]
        owner, place = lax.div(slot, per_owner), lax.rem(slot, per_owner)
        for part in range(halves):
            pltpu.make_async_copy(
                gathered_ref.at[owner * halves + part, place],
                mats[index].at[
                    pl.ds(row * side + part * half, half), pl.ds(col * side, side)
                ],
                sems.at[index],
            ).start()
    for index, matrix in enumerate(mats):
        pltpu.make_async_copy(matrix, matrix, sems.at[index]).wait()


def assemble(gathered, owner_slot, halves):
    shapes = matrix_shapes()
    return pl.pallas_call(
        functools.partial(assemble_body, gathered.shape[1], halves),
        in_specs=[
            pl.BlockSpec(memory_space=pltpu.SMEM),
            pl.BlockSpec(memory_space=pl.ANY),
        ],
        out_specs=[pl.BlockSpec(memory_space=pltpu.VMEM)] * len(shapes),
        out_shape=[jax.ShapeDtypeStruct(shape, gathered.dtype) for shape in shapes],
        scratch_shapes=[pltpu.SemaphoreType.DMA((len(shapes),))],
        cost_estimate=pl.CostEstimate(
            flops=0, bytes_accessed=4 * gathered.size, transcendentals=0
        ),
    )(owner_slot, gathered)


def deal_body(side, slot_ref, zero_ref, *refs):
    mats, (dealt_ref, used_ref, sem) = refs[:-3], refs[-3:]
    half = dealt_ref.shape[1]

    @pl.loop(0, dealt_ref.shape[0])
    def _(slot):
        used_ref[slot] = 0

    for block, (index, row, col) in enumerate(tile_walk(side)):
        slot = slot_ref[block]
        used_ref[slot] = 1
        pltpu.make_async_copy(
            mats[index].at[pl.ds(row * half, half), pl.ds(col * side, side)],
            dealt_ref.at[slot],
            sem,
        ).start()

    @pl.loop(0, dealt_ref.shape[0])
    def _(slot):
        @pl.when(used_ref[slot] == 0)
        def _():
            pltpu.make_async_copy(zero_ref, dealt_ref.at[slot], sem).start()

    pltpu.make_async_copy(dealt_ref, dealt_ref, sem).wait()


def deal(mats, owner_slot, slot_total, half, side):
    dtype = mats[0].dtype
    return pl.pallas_call(
        functools.partial(deal_body, side),
        in_specs=[pl.BlockSpec(memory_space=pltpu.SMEM)]
        + [pl.BlockSpec(memory_space=pltpu.VMEM)] * (1 + len(mats)),
        out_specs=pl.BlockSpec(memory_space=pl.ANY),
        out_shape=jax.ShapeDtypeStruct((slot_total, half, side), dtype),
        scratch_shapes=[pltpu.SMEM((slot_total,), jnp.int32), pltpu.SemaphoreType.DMA],
        cost_estimate=pl.CostEstimate(
            flops=0, bytes_accessed=4 * slot_total * half * side, transcendentals=0
        ),
    )(owner_slot, jnp.zeros((half, side), dtype), *mats)


MESH_IDS = pl.DeviceIdType.MESH


def spread_body(own_ref, out_ref, send_sem, recv_sem, local_sem):
    core, me = lax.axis_index("pair"), lax.axis_index("dp")
    level, rest = lax.div(me, 4), lax.rem(me, 4)
    flip_y = me + 2 - 4 * lax.div(rest, 2)
    flip_x = me + 1 - 2 * lax.rem(rest, 2)
    first = (1 - core) * flip_y + core * flip_x
    second = (1 - core) * flip_x + core * flip_y
    both = flip_x + flip_y - me
    targets = (
        (core, me + 4), (core, me - 4), (core, first), (core, second), (1 - core, me)
    )

    barrier = pltpu.get_barrier_semaphore()

    def greet(kind):
        pl.semaphore_signal(barrier, inc=1, device_id=targets[kind], device_id_type=MESH_IDS)

    @pl.when(level < 3)
    def _():
        greet(0)

    @pl.when(level > 0)
    def _():
        greet(1)

    for kind in (2, 3, 4):
        greet(kind)

    pl.semaphore_wait(barrier, 3 + lax.div(level + 3, 4) + lax.div(6 - level, 4))

    def link(kind, source, piece=None):
        place = source * 2 + core
        return pltpu.make_async_remote_copy(
            src_ref=out_ref.at[place] if piece is None else piece,
            dst_ref=out_ref.at[place],
            send_sem=send_sem.at[kind, source],
            recv_sem=recv_sem.at[kind // 4, source],
            device_id=targets[kind],
            device_id_type=MESH_IDS,
        )

    def walk(act):
        def line(base, step, kinds, up=(), down=()):
            @pl.when(level >= step)
            def _():
                act(base - 4 * step, kinds, up)

            @pl.when(level + step <= 3)
            def _():
                act(base + 4 * step, kinds, down)

        line(me, 1, (3, 2, 4), (0,), (1,))
        act(first, (3, 4), ())
        line(me, 2, (3, 2, 4), (0,), (1,))
        line(first, 1, (3, 4))
        line(me, 3, (3, 2, 4), (0,), (1,))
        line(first, 2, (3, 4))
        line(first, 3, (3, 4))
        act(second, (4,), ())
        line(second, 1, (4,))
        act(both, (4,), ())
        line(second, 2, (4,))
        line(both, 1, (4,))
        line(second, 3, (4,))
        line(both, 2, (4,))
        line(both, 3, (4,))

    def guarded(kind, run):
        if kind == 0:
            pl.when(level < 3)(run)
        elif kind == 1:
            pl.when(level > 0)(run)
        else:
            run()

    def go(source, kinds, further):
        link(0, source).wait_recv()
        for kind in further + kinds:
            guarded(kind, lambda kind=kind: link(kind, source).start())

    def drain(source, kinds, further):
        for kind in further + kinds:
            guarded(kind, lambda kind=kind: link(kind, source).wait_send())

    for kind in range(5):
        guarded(kind, lambda kind=kind: link(kind, me, own_ref).start())
    local = pltpu.make_async_copy(own_ref, out_ref.at[me * 2 + core], local_sem)
    local.start()
    walk(go)
    for kind in range(5):
        guarded(kind, lambda kind=kind: link(kind, me, own_ref).wait_send())
    walk(drain)

    @pl.loop(0, 16)
    def _(source):
        pltpu.make_async_remote_copy(
            src_ref=own_ref,
            dst_ref=out_ref.at[source * 2 + 1 - core],
            send_sem=send_sem.at[4, source],
            recv_sem=recv_sem.at[1, source],
            device_id=targets[4],
            device_id_type=MESH_IDS,
        ).wait_recv()

    local.wait()


def spread(own, data_count, pair_count):
    if (data_count, pair_count) != (16, 2):
        return lax.all_gather(own, ("dp", "pair"), axis=0)
    return pl.pallas_call(
        spread_body,
        in_specs=[pl.BlockSpec(memory_space=pl.ANY)],
        out_specs=pl.BlockSpec(memory_space=pl.ANY),
        out_shape=jax.ShapeDtypeStruct((32,) + own.shape, own.dtype),
        scratch_shapes=[
            pltpu.SemaphoreType.DMA((5, 16)),
            pltpu.SemaphoreType.DMA((2, 16)),
            pltpu.SemaphoreType.DMA,
        ],
        compiler_params=pltpu.CompilerParams(collective_id=1, has_side_effects=True),
    )(own)


def fold_body(own_ref, out_ref, land, send_sem, recv_sem):
    core, me = lax.axis_index("pair"), lax.axis_index("dp")
    level, rest = lax.div(me, 4), lax.rem(me, 4)
    flip_y = me + 2 - 4 * lax.div(rest, 2)
    flip_x = me + 1 - 2 * lax.rem(rest, 2)
    first = (1 - core) * flip_y + core * flip_x
    second = (1 - core) * flip_x + core * flip_y
    both = flip_x + flip_y - me
    targets = ((core, second), (core, second), (core, first), (core, me + 4), (core, me - 4))
    barrier = pltpu.get_barrier_semaphore()

    def greet(kind):
        pl.semaphore_signal(barrier, inc=1, device_id=targets[kind], device_id_type=MESH_IDS)

    @pl.when(level < 3)
    def _():
        greet(3)

    @pl.when(level > 0)
    def _():
        greet(4)

    greet(0)
    greet(2)
    pl.semaphore_wait(barrier, 2 + lax.div(level + 3, 4) + lax.div(6 - level, 4))

    def link(kind, place, source):
        return pltpu.make_async_remote_copy(
            src_ref=source,
            dst_ref=land.at[kind, place],
            send_sem=send_sem.at[kind, place],
            recv_sem=recv_sem.at[kind, place],
            device_id=targets[kind],
            device_id_type=MESH_IDS,
        )

    def landed(kind, place):
        link(kind, place, land.at[kind, place]).wait_recv()

    def levels(step, act):
        if step == 0:
            act(level, 0)
            return

        @pl.when(level >= step)
        def _():
            act(level - step, -1)

        @pl.when(level + step <= 3)
        def _():
            act(level + step, 1)

    def column(base, place):
        return base + 4 * (place - level)

    def total(piece, place, kinds, store):
        @pl.loop(0, own_ref.shape[1])
        def _(row):
            value = own_ref[piece, row].astype(jnp.float32)
            for kind in kinds:
                value = value + land[kind, place, row].astype(jnp.float32)
            store(row, value.astype(land.dtype))

    def send_second(kind, base):
        def act(place, side):
            link(kind, place, own_ref.at[column(base, place)]).start()

        return act

    def send_first(place, side):
        landed(1, place)

        def store(row, value):
            land[1, place, row] = value

        total(column(first, place), place, (1,), store)
        link(2, place, land.at[1, place]).start()

    def send_along(place, side):
        landed(0, place)
        landed(2, place)
        kind = 3 if side > 0 else 4
        ends = level == (0 if side > 0 else 3)

        def store(row, value):
            land[0, place, row] = value

        @pl.when(ends)
        def _():
            total(column(me, place), place, (0, 2), store)

        @pl.when(jnp.logical_not(ends))
        def _():
            landed(kind, place)
            total(column(me, place), place, (0, 2, kind), store)

        link(kind, place, land.at[0, place]).start()

    for step, kind in ((3, 1), (2, 1), (3, 0), (1, 1), (2, 0), (0, 1), (1, 0), (0, 0)):
        levels(step, send_second(kind, both if kind else second))
    levels(3, send_first)
    levels(2, send_first)
    levels(3, send_along)
    levels(1, send_first)
    levels(2, send_along)
    levels(0, send_first)
    levels(1, send_along)

    def keep(row, value):
        out_ref[row] = value

    landed(0, level)
    landed(2, level)

    @pl.when(level == 0)
    def _():
        landed(4, level)
        total(me, level, (0, 2, 4), keep)

    @pl.when(level == 3)
    def _():
        landed(3, level)
        total(me, level, (0, 2, 3), keep)

    @pl.when(jnp.logical_and(level > 0, level < 3))
    def _():
        landed(3, level)
        landed(4, level)
        total(me, level, (0, 2, 3, 4), keep)

    for step in range(4):
        for kind in range(3):
            levels(step, lambda place, side, kind=kind: link(kind, place, land.at[0, 0]).wait_send())
        if step:
            levels(
                step,
                lambda place, side: link(
                    3 if side > 0 else 4, place, land.at[0, 0]
                ).wait_send(),
            )


def fold(dealt, data_count, pair_count):
    if (data_count, pair_count) != (16, 2):
        return lax.psum_scatter(dealt, "dp", scatter_dimension=0, tiled=True)
    pieces = dealt.reshape((16, dealt.shape[0] // 16) + dealt.shape[1:])
    return pl.pallas_call(
        fold_body,
        in_specs=[pl.BlockSpec(memory_space=pltpu.VMEM)],
        out_specs=pl.BlockSpec(memory_space=pltpu.VMEM),
        out_shape=jax.ShapeDtypeStruct(pieces.shape[1:], dealt.dtype),
        scratch_shapes=[
            pltpu.VMEM((5, 4) + pieces.shape[1:], dealt.dtype),
            pltpu.SemaphoreType.DMA((5, 4)),
            pltpu.SemaphoreType.DMA((5, 4)),
        ],
        compiler_params=pltpu.CompilerParams(collective_id=2, has_side_effects=True),
    )(pieces)


def vector_body(rounds, part_ref, total_ref, held, landed, send_sem, recv_sem):
    core, me = lax.axis_index("pair"), lax.axis_index("dp")
    partners = [(1 - core, me)]
    for step in range(rounds - 1):
        bit = 2**step
        partners.append((core, me + bit - 2 * bit * lax.rem(lax.div(me, bit), 2)))
    barrier = pltpu.get_barrier_semaphore()
    for partner in partners:
        pl.semaphore_signal(barrier, inc=1, device_id=partner, device_id_type=MESH_IDS)
    pl.semaphore_wait(barrier, rounds)
    for step, partner in enumerate(partners):
        source = part_ref if step == 0 else held.at[step - 1]
        copy = pltpu.make_async_remote_copy(
            src_ref=source,
            dst_ref=landed.at[step],
            send_sem=send_sem.at[step],
            recv_sem=recv_sem.at[step],
            device_id=partner,
            device_id_type=MESH_IDS,
        )
        copy.start()
        copy.wait()
        total = source[...] + landed[step]
        if step < rounds - 1:
            held[step] = total
        else:
            total_ref[...] = total


def vector_total(part, data_count, pair_count):
    rounds = data_count.bit_length()
    if pair_count != 2 or 2 ** (rounds - 1) != data_count:
        return lax.psum(part, ("pair", "dp"))
    shape = (part.shape[0] // 128, 128)
    return pl.pallas_call(
        functools.partial(vector_body, rounds),
        in_specs=[pl.BlockSpec(memory_space=pltpu.VMEM)],
        out_specs=pl.BlockSpec(memory_space=pltpu.VMEM),
        out_shape=jax.ShapeDtypeStruct(shape, part.dtype),
        scratch_shapes=[
            pltpu.VMEM((rounds,) + shape, part.dtype),
            pltpu.VMEM((rounds,) + shape, part.dtype),
            pltpu.SemaphoreType.DMA((rounds,)),
            pltpu.SemaphoreType.DMA((rounds,)),
        ],
        compiler_params=pltpu.CompilerParams(collective_id=0, has_side_effects=True),
        cost_estimate=pl.CostEstimate(
            flops=part.size * rounds, bytes_accessed=8 * part.size * rounds, transcendentals=0
        ),
    )(part.reshape(shape)).reshape(-1)


def pair_summed(gradient, scale, block_side, core):
    halves = lax.axis_size("pair")
    half = block_side // halves
    gradient = (gradient * scale).astype(jnp.bfloat16)
    parts = gradient.reshape(-1, halves, half, gradient.shape[1])
    sent = lax.dynamic_index_in_dim(parts, 1 - core, axis=1, keepdims=False)
    kept = lax.dynamic_index_in_dim(parts, core, axis=1, keepdims=False)
    total = kept.astype(jnp.float32) + swapped(sent, "pair", 0).astype(jnp.float32)
    return total.astype(jnp.bfloat16).reshape(-1, gradient.shape[1])


def soap_update(gradient, weight, moment_one, moment_two, left_basis, right_basis):
    rotated = jnp.matmul(
        jnp.matmul(jnp.swapaxes(left_basis, -1, -2), gradient, precision=HIGHEST),
        right_basis,
        precision=HIGHEST,
    )
    moment_one = BETA_ONE * moment_one + (1.0 - BETA_ONE) * rotated
    moment_two = BETA_TWO * moment_two + (1.0 - BETA_TWO) * rotated * rotated
    direction = (
        moment_one
        / (1.0 - BETA_ONE**STEP)
        / (jnp.sqrt(moment_two / (1.0 - BETA_TWO**STEP)) + ADAM_EPS)
    )
    restored = jnp.matmul(
        jnp.matmul(left_basis, direction, precision=HIGHEST),
        jnp.swapaxes(right_basis, -1, -2),
        precision=HIGHEST,
    )
    return (weight - LR_MATRIX * (restored + DECAY_RATE * weight), moment_one, moment_two)


def adam_update(gradient, weight, moment_one, moment_two):
    moment_one = BETA_ONE * moment_one + (1.0 - BETA_ONE) * gradient
    moment_two = BETA_TWO * moment_two + (1.0 - BETA_TWO) * gradient * gradient
    direction = (
        moment_one
        / (1.0 - BETA_ONE**STEP)
        / (jnp.sqrt(moment_two / (1.0 - BETA_TWO**STEP)) + ADAM_EPS)
    )
    return (weight - LR_VECTOR * direction, moment_one, moment_two)


def scores_of(left, right):
    return lax.dot_general(
        left, right, (((1,), (1,)), ((), ())), preferred_element_type=jnp.float32
    )


def attend_forward_body(head_dim, seg_col, seg_row, q_ref, k_ref, v_ref, o_ref):
    allowed = seg_col[0] == seg_row[0]
    factor = 1.0 / math.sqrt(head_dim)
    for start in range(0, q_ref.shape[1], head_dim):
        lanes = slice(start, start + head_dim)
        scores = scores_of(q_ref[:, lanes], k_ref[:, lanes])
        scores = jnp.where(allowed, scores * factor, -1e30)
        top = jnp.max(scores, axis=1, keepdims=True)
        weights = jnp.exp(scores - top)
        total = jnp.sum(weights, axis=1, keepdims=True)
        probs = (weights * (1.0 / total)).astype(jnp.bfloat16)
        mixed = jnp.dot(probs, v_ref[:, lanes], preferred_element_type=jnp.float32)
        o_ref[:, lanes] = mixed.astype(o_ref.dtype)


def attend_backward_body(
    head_dim, seg_col, seg_row, q_ref, k_ref, v_ref, g_ref, dq_ref, dk_ref, dv_ref
):
    allowed = seg_col[0] == seg_row[0]
    factor = 1.0 / math.sqrt(head_dim)
    for start in range(0, q_ref.shape[1], head_dim):
        lanes = slice(start, start + head_dim)
        query, key = q_ref[:, lanes], k_ref[:, lanes]
        value, grad = v_ref[:, lanes], g_ref[:, lanes]
        scores = jnp.where(allowed, scores_of(key, query) * factor, -1e30)
        top = jnp.max(scores, axis=0, keepdims=True)
        weights = jnp.exp(scores - top)
        total = jnp.sum(weights, axis=0, keepdims=True)
        probs = weights * (1.0 / total)
        dv = jnp.dot(probs.astype(jnp.bfloat16), grad, preferred_element_type=jnp.float32)
        dv_ref[:, lanes] = dv.astype(dv_ref.dtype)
        grad_probs = scores_of(value, grad)
        inner = jnp.sum(probs * grad_probs, axis=0, keepdims=True)
        grad_scores = probs * (grad_probs - inner)
        grad_logits = jnp.where(allowed, grad_scores * factor, 0.0).astype(jnp.bfloat16)
        dk = jnp.dot(grad_logits, query, preferred_element_type=jnp.float32)
        dk_ref[:, lanes] = dk.astype(dk_ref.dtype)
        dq = lax.dot_general(
            grad_logits, key, (((0,), (0,)), ((), ())), preferred_element_type=jnp.float32
        )
        dq_ref[:, lanes] = dq.astype(dq_ref.dtype)


def attention_call(body, count_out, segment_id, arrays):
    rows, seq_len = segment_id.shape
    width = arrays[0].shape[1]
    lanes = 2 * (D // HEADS)
    tile = pl.BlockSpec((seq_len, lanes), lambda r, h: (r, h))
    shape = jax.ShapeDtypeStruct(arrays[0].shape, jnp.bfloat16)
    flops = 2 * rows * seq_len * seq_len * width * (2 if count_out == 1 else 5)
    return pl.pallas_call(
        functools.partial(body, D // HEADS),
        grid=(rows, width // lanes),
        in_specs=[
            pl.BlockSpec((1, seq_len, 1), lambda r, h: (r, 0, 0)),
            pl.BlockSpec((1, 1, seq_len), lambda r, h: (r, 0, 0)),
        ]
        + [tile] * len(arrays),
        out_specs=[tile] * count_out,
        out_shape=[shape] * count_out,
        cost_estimate=pl.CostEstimate(
            flops=flops,
            bytes_accessed=2 * arrays[0].size * (len(arrays) + count_out),
            transcendentals=rows * HEADS * seq_len * seq_len,
        ),
    )(segment_id[:, :, None], segment_id[:, None, :], *arrays)


def per_device(
    inputs,
    cotangent,
    span_lengths,
    pad_lengths,
    pairing,
    owner_slot,
    master,
    first_moment,
    second_moment,
    left_basis,
    right_basis,
    vector_master,
    vector_first,
    vector_second,
):
    pair_count = lax.axis_size("pair")
    data_count = lax.axis_size("dp")
    grad_scale = 1.0 / (pair_count * data_count)
    block_side = master.shape[-1]
    half = block_side // pair_count
    core = lax.axis_index("pair")
    own_half = lax.dynamic_slice_in_dim(master, core * half, half, axis=1).astype(jnp.bfloat16)
    gathered = spread(own_half, data_count, pair_count)
    w_query, w_key, w_value, w_output, w_inner, w_outer = assemble(
        gathered, owner_slot, pair_count
    )
    (
        gain_one,
        shift_one,
        gain_two,
        shift_two,
        bias_query,
        bias_value,
        bias_output,
        bias_outer,
        bias_inner,
    ) = split_vector(vector_master)
    row_count = inputs.shape[1]
    seq_len = inputs.shape[2]
    token_count = row_count * seq_len
    flat_input = inputs.reshape(token_count, D)
    span_rows = span_lengths[0]
    pad_rows = pad_lengths[0]
    span_ends = jnp.cumsum(span_rows, axis=-1)
    span_starts = span_ends - span_rows
    positions = jnp.arange(seq_len, dtype=jnp.int32)
    inside = jnp.sum(
        (positions[None, :, None] >= span_ends[:, None, :-1]).astype(jnp.int32), axis=-1
    )
    segment_id = jnp.where(positions[None, :] >= seq_len - pad_rows[:, None], SEGS, inside)
    query_rows = (
        (jnp.dot(flat_input, w_query, preferred_element_type=jnp.float32) + bias_query)
        .astype(jnp.bfloat16)
    )
    key_rows = (
        jnp.dot(flat_input, w_key, preferred_element_type=jnp.float32)
        .astype(jnp.bfloat16)
    )
    value_rows = (
        (jnp.dot(flat_input, w_value, preferred_element_type=jnp.float32) + bias_value)
        .astype(jnp.bfloat16)
    )
    (mixed_low,) = attention_call(
        attend_forward_body, 1, segment_id, (query_rows, key_rows, value_rows)
    )
    branch = jnp.dot(mixed_low, w_output, preferred_element_type=jnp.float32) + bias_output
    residual_one = flat_input.astype(jnp.float32) + branch
    normed = layer_norm(residual_one, gain_one, shift_one)
    normed_low = normed.astype(jnp.bfloat16)
    inner_sum = jnp.dot(normed_low, w_inner, preferred_element_type=jnp.float32) + bias_inner
    active, slope = gelu_and_slope(inner_sum)
    active_low, slope_low = active.astype(jnp.bfloat16), slope.astype(jnp.bfloat16)
    outer_sum = jnp.dot(active_low, w_outer, preferred_element_type=jnp.float32) + bias_outer
    residual_two = normed + outer_sum
    result = layer_norm(residual_two, gain_two, shift_two)
    result_rows = result.reshape(row_count, seq_len, D)
    leaders = jnp.take_along_axis(result_rows, span_starts[:, :, None], axis=1).reshape(-1, D)
    partner = swapped(leaders.astype(jnp.bfloat16), "pair", 0).astype(jnp.float32)
    pair_logits = (
        jnp.dot(leaders, partner.T, precision=HIGHEST, preferred_element_type=jnp.float32)
        * CLS_SCALE
    )
    pair_probs = jax.nn.softmax(pair_logits, axis=-1)
    targets = (
        pairing.reshape(-1)[:, None] == jnp.arange(leaders.shape[0], dtype=jnp.int32)[None, :]
    ).astype(jnp.float32)
    grad_pair = CLS_WEIGHT * CLS_SCALE * (pair_probs - targets)
    grad_leaders = jnp.dot(
        grad_pair, partner, precision=HIGHEST, preferred_element_type=jnp.float32
    )
    grad_partner = jnp.dot(
        grad_pair.T, leaders, precision=HIGHEST, preferred_element_type=jnp.float32
    )
    returned = swapped(grad_partner.astype(jnp.bfloat16), "pair", 0).astype(jnp.float32)
    grad_leaders = grad_leaders + returned
    valid_mask = (segment_id < SEGS).astype(jnp.float32)
    grad_result = cotangent[0].astype(jnp.float32) * valid_mask[:, :, None]
    row_index = jnp.arange(row_count, dtype=jnp.int32)[:, None]
    grad_result = grad_result.at[row_index, span_starts].add(
        grad_leaders.reshape(row_count, SEGS, D)
    )
    grad_result = grad_result.reshape(token_count, D)
    primal_two, norm_two_back = jax.vjp(layer_norm, residual_two, gain_two, shift_two)
    grad_residual_two, grad_gain_two, grad_shift_two = norm_two_back(grad_result)
    grad_outer = grad_residual_two.astype(jnp.bfloat16)
    grad_bias_outer = jnp.sum(grad_outer, axis=0, dtype=jnp.float32)
    grad_w_outer = jnp.einsum(
        "tf,td->fd", active_low, grad_outer, preferred_element_type=jnp.float32
    )
    grad_active = jnp.einsum("td,fd->tf", grad_outer, w_outer, preferred_element_type=jnp.float32)
    grad_inner = (grad_active * slope_low.astype(jnp.float32)).astype(jnp.bfloat16)
    grad_bias_inner = jnp.sum(grad_inner, axis=0, dtype=jnp.float32)
    grad_w_inner = jnp.einsum(
        "td,tf->df", normed_low, grad_inner, preferred_element_type=jnp.float32
    )
    grad_normed = grad_residual_two + jnp.einsum(
        "tf,df->td", grad_inner, w_inner, preferred_element_type=jnp.float32
    )
    primal_one, norm_one_back = jax.vjp(layer_norm, residual_one, gain_one, shift_one)
    grad_residual_one, grad_gain_one, grad_shift_one = norm_one_back(grad_normed)
    grad_branch = grad_residual_one.astype(jnp.bfloat16)
    grad_bias_output = jnp.sum(grad_branch, axis=0, dtype=jnp.float32)
    grad_w_output = jnp.einsum(
        "td,te->de", mixed_low, grad_branch, preferred_element_type=jnp.float32
    )
    grad_mixed = (
        jnp.einsum("te,de->td", grad_branch, w_output, preferred_element_type=jnp.float32)
        .astype(jnp.bfloat16)
    )
    grad_query, grad_key, grad_value = attention_call(
        attend_backward_body, 3, segment_id, (query_rows, key_rows, value_rows, grad_mixed)
    )
    grad_bias_query = jnp.sum(grad_query, axis=0, dtype=jnp.float32)
    grad_bias_value = jnp.sum(grad_value, axis=0, dtype=jnp.float32)
    grad_w_query = jnp.einsum(
        "td,te->de", flat_input, grad_query, preferred_element_type=jnp.float32
    )
    grad_w_key = jnp.einsum("td,te->de", flat_input, grad_key, preferred_element_type=jnp.float32)
    grad_w_value = jnp.einsum(
        "td,te->de", flat_input, grad_value, preferred_element_type=jnp.float32
    )
    grad_inputs = grad_residual_one + jnp.einsum(
        "te,de->td", grad_query, w_query, preferred_element_type=jnp.float32
    )
    grad_inputs = grad_inputs + jnp.einsum(
        "te,de->td", grad_key, w_key, preferred_element_type=jnp.float32
    )
    grad_inputs = grad_inputs + jnp.einsum(
        "te,de->td", grad_value, w_value, preferred_element_type=jnp.float32
    )
    local_vector = (
        jnp.concatenate(
            [
                grad_gain_one,
                grad_shift_one,
                grad_gain_two,
                grad_shift_two,
                grad_bias_query,
                grad_bias_value,
                grad_bias_output,
                grad_bias_outer,
                grad_bias_inner,
            ]
        )
        * grad_scale
    )
    grad_mats = [
        pair_summed(matrix, grad_scale, block_side, core)
        for matrix in (
            grad_w_query, grad_w_key, grad_w_value, grad_w_output, grad_w_inner, grad_w_outer
        )
    ]
    own_grad = deal(grad_mats, owner_slot, master.shape[0] * data_count, half, block_side)
    vector_grad = vector_total(local_vector, data_count, pair_count)
    own_grad = fold(own_grad, data_count, pair_count)
    owned_grad = lax.all_gather(own_grad, "pair", axis=1, tiled=True).astype(jnp.float32)
    new_master, new_first, new_second = soap_update(
        owned_grad, master, first_moment, second_moment, left_basis, right_basis
    )
    new_vector, vector_one, vector_two = adam_update(
        vector_grad, vector_master, vector_first, vector_second
    )
    return (
        result_rows.astype(jnp.bfloat16).reshape(inputs.shape),
        grad_inputs.reshape(inputs.shape),
        owned_grad,
        new_master,
        new_first,
        new_second,
        vector_grad,
        jnp.stack([new_vector, vector_one, vector_two], axis=0),
    )


def solution(mesh):
    placed = (
        P("pair", "dp", None, None),
        P("pair", "dp", None, None),
        P("pair", "dp", None),
        P("pair", "dp"),
        P("pair", "dp", None),
        P(),
        P("dp", None, None),
        P("dp", None, None),
        P("dp", None, None),
        P("dp", None, None),
        P("dp", None, None),
        P(),
        P(),
        P(),
    )
    return jax.shard_map(
        per_device,
        mesh=mesh,
        in_specs=placed,
        out_specs=(
            P("pair", "dp", None, None),
            P("pair", "dp", None, None),
            P("dp", None, None),
            P("dp", None, None),
            P("dp", None, None),
            P("dp", None, None),
            P(),
            P(),
        ),
        check_vma=False,
    )
```

```python
import functools
import math

import jax
import jax.numpy as jnp
from jax import lax
from jax.experimental import pallas as pl
from jax.experimental.pallas import tpu as pltpu
from jax.sharding import PartitionSpec as P

D = 768
HEADS = 12
FF = 3072
SEGS = 4
STEP = 10


HIGHEST = lax.Precision.HIGHEST
BETA_ONE = 0.9
BETA_TWO = 0.95
ADAM_EPS = 1e-08
LR_MATRIX = 0.1
LR_VECTOR = 1.0
DECAY_RATE = 0.01
NORM_EPS = 1e-12
CLS_SCALE = 0.0625
CLS_WEIGHT = 4.0


def swapped(array, axis, stride):
    return lax.ppermute(array, axis, [(i, i ^ 1 << stride) for i in range(lax.axis_size(axis))])


def layer_norm(values, gain_vector, shift_vector):
    average = jnp.mean(values, axis=-1, keepdims=True)
    centered = values - average
    variance = jnp.mean(centered * centered, axis=-1, keepdims=True)
    return centered * lax.rsqrt(variance + NORM_EPS) * gain_vector + shift_vector


def gelu_and_slope(values):
    lower = 0.5 * (1.0 + lax.erf(values * math.sqrt(0.5)))
    density = jnp.exp(-0.5 * values * values) * (1.0 / math.sqrt(2.0 * math.pi))
    return values * lower, lower + values * density


def split_vector(vector):
    pieces = [vector[index * D : (index + 1) * D] for index in range(8)]
    return tuple(pieces) + (vector[8 * D : 8 * D + FF],)


def matrix_shapes():
    return ((D, D),) * 4 + ((D, FF), (FF, D))


def tile_walk(block_side):
    for index, (rows, cols) in enumerate(matrix_shapes()):
        for row in range(rows // block_side):
            for col in range(cols // block_side):
                yield index, row, col


def assemble_body(per_owner, halves, slot_ref, gathered_ref, *refs):
    mats, sems = refs[:-1], refs[-1]
    half, side = gathered_ref.shape[-2:]
    for block, (index, row, col) in enumerate(tile_walk(side)):
        slot = slot_ref[block]
        owner, place = lax.div(slot, per_owner), lax.rem(slot, per_owner)
        for part in range(halves):
            pltpu.make_async_copy(
                gathered_ref.at[owner * halves + part, place],
                mats[index].at[
                    pl.ds(row * side + part * half, half), pl.ds(col * side, side)
                ],
                sems.at[index],
            ).start()
    for index, matrix in enumerate(mats):
        pltpu.make_async_copy(matrix, matrix, sems.at[index]).wait()


def assemble(gathered, owner_slot, halves):
    shapes = matrix_shapes()
    return pl.pallas_call(
        functools.partial(assemble_body, gathered.shape[1], halves),
        in_specs=[
            pl.BlockSpec(memory_space=pltpu.SMEM),
            pl.BlockSpec(memory_space=pl.ANY),
        ],
        out_specs=[pl.BlockSpec(memory_space=pltpu.VMEM)] * len(shapes),
        out_shape=[jax.ShapeDtypeStruct(shape, gathered.dtype) for shape in shapes],
        scratch_shapes=[pltpu.SemaphoreType.DMA((len(shapes),))],
        cost_estimate=pl.CostEstimate(
            flops=0, bytes_accessed=4 * gathered.size, transcendentals=0
        ),
    )(owner_slot, gathered)


def deal_body(side, slot_ref, zero_ref, *refs):
    mats, (dealt_ref, used_ref, sem) = refs[:-3], refs[-3:]
    half = dealt_ref.shape[1]

    @pl.loop(0, dealt_ref.shape[0])
    def _(slot):
        used_ref[slot] = 0

    for block, (index, row, col) in enumerate(tile_walk(side)):
        slot = slot_ref[block]
        used_ref[slot] = 1
        pltpu.make_async_copy(
            mats[index].at[pl.ds(row * half, half), pl.ds(col * side, side)],
            dealt_ref.at[slot],
            sem,
        ).start()

    @pl.loop(0, dealt_ref.shape[0])
    def _(slot):
        @pl.when(used_ref[slot] == 0)
        def _():
            pltpu.make_async_copy(zero_ref, dealt_ref.at[slot], sem).start()

    pltpu.make_async_copy(dealt_ref, dealt_ref, sem).wait()


def deal(mats, owner_slot, slot_total, half, side):
    dtype = mats[0].dtype
    return pl.pallas_call(
        functools.partial(deal_body, side),
        in_specs=[pl.BlockSpec(memory_space=pltpu.SMEM)]
        + [pl.BlockSpec(memory_space=pltpu.VMEM)] * (1 + len(mats)),
        out_specs=pl.BlockSpec(memory_space=pl.ANY),
        out_shape=jax.ShapeDtypeStruct((slot_total, half, side), dtype),
        scratch_shapes=[pltpu.SMEM((slot_total,), jnp.int32), pltpu.SemaphoreType.DMA],
        cost_estimate=pl.CostEstimate(
            flops=0, bytes_accessed=4 * slot_total * half * side, transcendentals=0
        ),
    )(owner_slot, jnp.zeros((half, side), dtype), *mats)


MESH_IDS = pl.DeviceIdType.MESH


def spread_body(own_ref, out_ref, send_sem, recv_sem, local_sem):
    core, me = lax.axis_index("pair"), lax.axis_index("dp")
    level, rest = lax.div(me, 4), lax.rem(me, 4)
    flip_y = me + 2 - 4 * lax.div(rest, 2)
    flip_x = me + 1 - 2 * lax.rem(rest, 2)
    first = (1 - core) * flip_y + core * flip_x
    second = (1 - core) * flip_x + core * flip_y
    both = flip_x + flip_y - me
    targets = (
        (core, me + 4), (core, me - 4), (core, first), (core, second), (1 - core, me)
    )

    barrier = pltpu.get_barrier_semaphore()

    def greet(kind):
        pl.semaphore_signal(barrier, inc=1, device_id=targets[kind], device_id_type=MESH_IDS)

    @pl.when(level < 3)
    def _():
        greet(0)

    @pl.when(level > 0)
    def _():
        greet(1)

    for kind in (2, 3, 4):
        greet(kind)

    pl.semaphore_wait(barrier, 3 + lax.div(level + 3, 4) + lax.div(6 - level, 4))

    def link(kind, source, piece=None):
        place = source * 2 + core
        return pltpu.make_async_remote_copy(
            src_ref=out_ref.at[place] if piece is None else piece,
            dst_ref=out_ref.at[place],
            send_sem=send_sem.at[kind, source],
            recv_sem=recv_sem.at[kind // 4, source],
            device_id=targets[kind],
            device_id_type=MESH_IDS,
        )

    def walk(act):
        def line(base, step, kinds, up=(), down=()):
            @pl.when(level >= step)
            def _():
                act(base - 4 * step, kinds, up)

            @pl.when(level + step <= 3)
            def _():
                act(base + 4 * step, kinds, down)

        line(me, 1, (3, 2, 4), (0,), (1,))
        act(first, (3, 4), ())
        line(me, 2, (3, 2, 4), (0,), (1,))
        line(first, 1, (3, 4))
        line(me, 3, (3, 2, 4), (0,), (1,))
        line(first, 2, (3, 4))
        line(first, 3, (3, 4))
        act(second, (4,), ())
        line(second, 1, (4,))
        act(both, (4,), ())
        line(second, 2, (4,))
        line(both, 1, (4,))
        line(second, 3, (4,))
        line(both, 2, (4,))
        line(both, 3, (4,))

    def guarded(kind, run):
        if kind == 0:
            pl.when(level < 3)(run)
        elif kind == 1:
            pl.when(level > 0)(run)
        else:
            run()

    def go(source, kinds, further):
        link(0, source).wait_recv()
        for kind in further + kinds:
            guarded(kind, lambda kind=kind: link(kind, source).start())

    def drain(source, kinds, further):
        for kind in further + kinds:
            guarded(kind, lambda kind=kind: link(kind, source).wait_send())

    for kind in range(5):
        guarded(kind, lambda kind=kind: link(kind, me, own_ref).start())
    local = pltpu.make_async_copy(own_ref, out_ref.at[me * 2 + core], local_sem)
    local.start()
    walk(go)
    for kind in range(5):
        guarded(kind, lambda kind=kind: link(kind, me, own_ref).wait_send())
    walk(drain)

    @pl.loop(0, 16)
    def _(source):
        pltpu.make_async_remote_copy(
            src_ref=own_ref,
            dst_ref=out_ref.at[source * 2 + 1 - core],
            send_sem=send_sem.at[4, source],
            recv_sem=recv_sem.at[1, source],
            device_id=targets[4],
            device_id_type=MESH_IDS,
        ).wait_recv()

    local.wait()


def spread(own, data_count, pair_count):
    if (data_count, pair_count) != (16, 2):
        return lax.all_gather(own, ("dp", "pair"), axis=0)
    return pl.pallas_call(
        spread_body,
        in_specs=[pl.BlockSpec(memory_space=pl.ANY)],
        out_specs=pl.BlockSpec(memory_space=pl.ANY),
        out_shape=jax.ShapeDtypeStruct((32,) + own.shape, own.dtype),
        scratch_shapes=[
            pltpu.SemaphoreType.DMA((5, 16)),
            pltpu.SemaphoreType.DMA((2, 16)),
            pltpu.SemaphoreType.DMA,
        ],
        compiler_params=pltpu.CompilerParams(collective_id=1, has_side_effects=True),
    )(own)


def fold_body(own_ref, out_ref, land, send_sem, recv_sem):
    core, me = lax.axis_index("pair"), lax.axis_index("dp")
    level, rest = lax.div(me, 4), lax.rem(me, 4)
    flip_y = me + 2 - 4 * lax.div(rest, 2)
    flip_x = me + 1 - 2 * lax.rem(rest, 2)
    first = (1 - core) * flip_y + core * flip_x
    second = (1 - core) * flip_x + core * flip_y
    both = flip_x + flip_y - me
    targets = ((core, second), (core, second), (core, first), (core, me + 4), (core, me - 4))
    barrier = pltpu.get_barrier_semaphore()

    def greet(kind):
        pl.semaphore_signal(barrier, inc=1, device_id=targets[kind], device_id_type=MESH_IDS)

    @pl.when(level < 3)
    def _():
        greet(3)

    @pl.when(level > 0)
    def _():
        greet(4)

    greet(0)
    greet(2)
    pl.semaphore_wait(barrier, 2 + lax.div(level + 3, 4) + lax.div(6 - level, 4))

    def link(kind, place, source):
        return pltpu.make_async_remote_copy(
            src_ref=source,
            dst_ref=land.at[kind, place],
            send_sem=send_sem.at[kind, place],
            recv_sem=recv_sem.at[kind, place],
            device_id=targets[kind],
            device_id_type=MESH_IDS,
        )

    def landed(kind, place):
        link(kind, place, land.at[kind, place]).wait_recv()

    def levels(step, act):
        if step == 0:
            act(level, 0)
            return

        @pl.when(level >= step)
        def _():
            act(level - step, -1)

        @pl.when(level + step <= 3)
        def _():
            act(level + step, 1)

    def column(base, place):
        return base + 4 * (place - level)

    def total(piece, place, kinds, store):
        @pl.loop(0, own_ref.shape[1])
        def _(row):
            value = own_ref[piece, row].astype(jnp.float32)
            for kind in kinds:
                value = value + land[kind, place, row].astype(jnp.float32)
            store(row, value.astype(land.dtype))

    def send_second(kind, base):
        def act(place, side):
            link(kind, place, own_ref.at[column(base, place)]).start()

        return act

    def send_first(place, side):
        landed(1, place)

        def store(row, value):
            land[1, place, row] = value

        total(column(first, place), place, (1,), store)
        link(2, place, land.at[1, place]).start()

    def send_along(place, side):
        landed(0, place)
        landed(2, place)
        kind = 3 if side > 0 else 4
        ends = level == (0 if side > 0 else 3)

        def store(row, value):
            land[0, place, row] = value

        @pl.when(ends)
        def _():
            total(column(me, place), place, (0, 2), store)

        @pl.when(jnp.logical_not(ends))
        def _():
            landed(kind, place)
            total(column(me, place), place, (0, 2, kind), store)

        link(kind, place, land.at[0, place]).start()

    for step, kind in ((3, 1), (2, 1), (3, 0), (1, 1), (2, 0), (0, 1), (1, 0), (0, 0)):
        levels(step, send_second(kind, both if kind else second))
    levels(3, send_first)
    levels(2, send_first)
    levels(3, send_along)
    levels(1, send_first)
    levels(2, send_along)
    levels(0, send_first)
    levels(1, send_along)

    def keep(row, value):
        out_ref[row] = value

    landed(0, level)
    landed(2, level)

    @pl.when(level == 0)
    def _():
        landed(4, level)
        total(me, level, (0, 2, 4), keep)

    @pl.when(level == 3)
    def _():
        landed(3, level)
        total(me, level, (0, 2, 3), keep)

    @pl.when(jnp.logical_and(level > 0, level < 3))
    def _():
        landed(3, level)
        landed(4, level)
        total(me, level, (0, 2, 3, 4), keep)

    for step in range(4):
        for kind in range(3):
            levels(step, lambda place, side, kind=kind: link(kind, place, land.at[0, 0]).wait_send())
        if step:
            levels(
                step,
                lambda place, side: link(
                    3 if side > 0 else 4, place, land.at[0, 0]
                ).wait_send(),
            )


def fold(dealt, data_count, pair_count):
    if (data_count, pair_count) != (16, 2):
        return lax.psum_scatter(dealt, "dp", scatter_dimension=0, tiled=True)
    pieces = dealt.reshape((16, dealt.shape[0] // 16) + dealt.shape[1:])
    return pl.pallas_call(
        fold_body,
        in_specs=[pl.BlockSpec(memory_space=pltpu.VMEM)],
        out_specs=pl.BlockSpec(memory_space=pltpu.VMEM),
        out_shape=jax.ShapeDtypeStruct(pieces.shape[1:], dealt.dtype),
        scratch_shapes=[
            pltpu.VMEM((5, 4) + pieces.shape[1:], dealt.dtype),
            pltpu.SemaphoreType.DMA((5, 4)),
            pltpu.SemaphoreType.DMA((5, 4)),
        ],
        compiler_params=pltpu.CompilerParams(collective_id=2, has_side_effects=True),
    )(pieces)


def pair_body(half, count, *refs):
    mats, outs, lands = refs[:count], refs[count : 2 * count], refs[2 * count : 3 * count]
    send_sem, recv_sem, own_sem = refs[3 * count :]
    core, me = lax.axis_index("pair"), lax.axis_index("dp")
    target = (1 - core, me)
    barrier = pltpu.get_barrier_semaphore()
    pl.semaphore_signal(barrier, inc=1, device_id=target, device_id_type=MESH_IDS)
    pl.semaphore_wait(barrier, 1)
    stripes = []
    for index in range(count):
        for row in range(outs[index].shape[0] // half):
            number = len(stripes)
            here = pl.ds(row * half, half)

            def rows_of(part, row=row):
                return pl.ds(pl.multiple_of((2 * row + part) * half, half), half)

            remote = pltpu.make_async_remote_copy(
                src_ref=mats[index].at[rows_of(1 - core)],
                dst_ref=lands[index].at[here],
                send_sem=send_sem.at[number],
                recv_sem=recv_sem.at[number],
                device_id=target,
                device_id_type=MESH_IDS,
            )
            remote.start()
            own = pltpu.make_async_copy(
                mats[index].at[rows_of(core)], outs[index].at[here], own_sem.at[number]
            )
            own.start()
            stripes.append((index, row, remote, own))
    for index, row, remote, own in stripes:
        own.wait()
        remote.wait()
        out, land = outs[index], lands[index]

        @pl.loop(0, half // 16)
        def _(step, out=out, land=land, row=row):
            rows = pl.ds(pl.multiple_of(row * half + step * 16, 16), 16)
            total = out[rows, :].astype(jnp.float32) + land[rows, :].astype(jnp.float32)
            out[rows, :] = total.astype(out.dtype)


def pair_summed(mats, half):
    count = len(mats)
    shapes = [(matrix.shape[0] // 2, matrix.shape[1]) for matrix in mats]
    stripes = sum(shape[0] // half for shape in shapes)
    return pl.pallas_call(
        functools.partial(pair_body, half, count),
        in_specs=[pl.BlockSpec(memory_space=pl.ANY)] * count,
        out_specs=[pl.BlockSpec(memory_space=pltpu.VMEM)] * count,
        out_shape=[jax.ShapeDtypeStruct(shape, mats[0].dtype) for shape in shapes],
        scratch_shapes=[pltpu.VMEM(shape, mats[0].dtype) for shape in shapes]
        + [pltpu.SemaphoreType.DMA((stripes,))] * 3,
        compiler_params=pltpu.CompilerParams(collective_id=3, has_side_effects=True),
    )(*mats)


def vector_body(rounds, part_ref, total_ref, held, landed, send_sem, recv_sem):
    core, me = lax.axis_index("pair"), lax.axis_index("dp")
    partners = [(1 - core, me)]
    for step in range(rounds - 1):
        bit = 2**step
        partners.append((core, me + bit - 2 * bit * lax.rem(lax.div(me, bit), 2)))
    barrier = pltpu.get_barrier_semaphore()
    for partner in partners:
        pl.semaphore_signal(barrier, inc=1, device_id=partner, device_id_type=MESH_IDS)
    pl.semaphore_wait(barrier, rounds)
    for step, partner in enumerate(partners):
        source = part_ref if step == 0 else held.at[step - 1]
        copy = pltpu.make_async_remote_copy(
            src_ref=source,
            dst_ref=landed.at[step],
            send_sem=send_sem.at[step],
            recv_sem=recv_sem.at[step],
            device_id=partner,
            device_id_type=MESH_IDS,
        )
        copy.start()
        copy.wait()
        total = source[...] + landed[step]
        if step < rounds - 1:
            held[step] = total
        else:
            total_ref[...] = total


def vector_total(part, data_count, pair_count):
    rounds = data_count.bit_length()
    if pair_count != 2 or 2 ** (rounds - 1) != data_count:
        return lax.psum(part, ("pair", "dp"))
    shape = (part.shape[0] // 128, 128)
    return pl.pallas_call(
        functools.partial(vector_body, rounds),
        in_specs=[pl.BlockSpec(memory_space=pltpu.VMEM)],
        out_specs=pl.BlockSpec(memory_space=pltpu.VMEM),
        out_shape=jax.ShapeDtypeStruct(shape, part.dtype),
        scratch_shapes=[
            pltpu.VMEM((rounds,) + shape, part.dtype),
            pltpu.VMEM((rounds,) + shape, part.dtype),
            pltpu.SemaphoreType.DMA((rounds,)),
            pltpu.SemaphoreType.DMA((rounds,)),
        ],
        compiler_params=pltpu.CompilerParams(collective_id=0, has_side_effects=True),
        cost_estimate=pl.CostEstimate(
            flops=part.size * rounds, bytes_accessed=8 * part.size * rounds, transcendentals=0
        ),
    )(part.reshape(shape)).reshape(-1)


def soap_update(gradient, weight, moment_one, moment_two, left_basis, right_basis):
    rotated = jnp.matmul(
        jnp.matmul(jnp.swapaxes(left_basis, -1, -2), gradient, precision=HIGHEST),
        right_basis,
        precision=HIGHEST,
    )
    moment_one = BETA_ONE * moment_one + (1.0 - BETA_ONE) * rotated
    moment_two = BETA_TWO * moment_two + (1.0 - BETA_TWO) * rotated * rotated
    direction = (
        moment_one
        / (1.0 - BETA_ONE**STEP)
        / (jnp.sqrt(moment_two / (1.0 - BETA_TWO**STEP)) + ADAM_EPS)
    )
    restored = jnp.matmul(
        jnp.matmul(left_basis, direction, precision=HIGHEST),
        jnp.swapaxes(right_basis, -1, -2),
        precision=HIGHEST,
    )
    return (weight - LR_MATRIX * (restored + DECAY_RATE * weight), moment_one, moment_two)


def adam_update(gradient, weight, moment_one, moment_two):
    moment_one = BETA_ONE * moment_one + (1.0 - BETA_ONE) * gradient
    moment_two = BETA_TWO * moment_two + (1.0 - BETA_TWO) * gradient * gradient
    direction = (
        moment_one
        / (1.0 - BETA_ONE**STEP)
        / (jnp.sqrt(moment_two / (1.0 - BETA_TWO**STEP)) + ADAM_EPS)
    )
    return (weight - LR_VECTOR * direction, moment_one, moment_two)


def scores_of(left, right):
    return lax.dot_general(
        left, right, (((1,), (1,)), ((), ())), preferred_element_type=jnp.float32
    )


def attend_forward_body(head_dim, seg_col, seg_row, q_ref, k_ref, v_ref, o_ref):
    allowed = seg_col[0] == seg_row[0]
    factor = 1.0 / math.sqrt(head_dim)
    for start in range(0, q_ref.shape[1], head_dim):
        lanes = slice(start, start + head_dim)
        scores = scores_of(k_ref[:, lanes], q_ref[:, lanes])
        scores = jnp.where(allowed, scores * factor, -1e30)
        top = jnp.max(scores, axis=0, keepdims=True)
        weights = jnp.exp(scores - top)
        total = jnp.sum(weights, axis=0, keepdims=True)
        probs = (weights * (1.0 / total)).astype(jnp.bfloat16)
        mixed = lax.dot_general(
            probs, v_ref[:, lanes], (((0,), (0,)), ((), ())), preferred_element_type=jnp.float32
        )
        o_ref[:, lanes] = mixed.astype(o_ref.dtype)


def attend_backward_body(
    head_dim, seg_col, seg_row, q_ref, k_ref, v_ref, g_ref, dq_ref, dk_ref, dv_ref
):
    allowed = seg_col[0] == seg_row[0]
    factor = 1.0 / math.sqrt(head_dim)
    for start in range(0, q_ref.shape[1], head_dim):
        lanes = slice(start, start + head_dim)
        query, key = q_ref[:, lanes], k_ref[:, lanes]
        value, grad = v_ref[:, lanes], g_ref[:, lanes]
        scores = jnp.where(allowed, scores_of(key, query) * factor, -1e30)
        top = jnp.max(scores, axis=0, keepdims=True)
        weights = jnp.exp(scores - top)
        total = jnp.sum(weights, axis=0, keepdims=True)
        probs = weights * (1.0 / total)
        dv = jnp.dot(probs.astype(jnp.bfloat16), grad, preferred_element_type=jnp.float32)
        dv_ref[:, lanes] = dv.astype(dv_ref.dtype)
        grad_probs = scores_of(value, grad)
        inner = jnp.sum(probs * grad_probs, axis=0, keepdims=True)
        grad_scores = probs * (grad_probs - inner)
        grad_logits = jnp.where(allowed, grad_scores * factor, 0.0).astype(jnp.bfloat16)
        dk = jnp.dot(grad_logits, query, preferred_element_type=jnp.float32)
        dk_ref[:, lanes] = dk.astype(dk_ref.dtype)
        dq = lax.dot_general(
            grad_logits, key, (((0,), (0,)), ((), ())), preferred_element_type=jnp.float32
        )
        dq_ref[:, lanes] = dq.astype(dq_ref.dtype)


def attention_call(body, count_out, segment_id, arrays):
    rows, seq_len = segment_id.shape
    width = arrays[0].shape[1]
    lanes = 2 * (D // HEADS)
    tile = pl.BlockSpec((seq_len, lanes), lambda r, h: (r, h))
    shape = jax.ShapeDtypeStruct(arrays[0].shape, jnp.bfloat16)
    flops = 2 * rows * seq_len * seq_len * width * (2 if count_out == 1 else 5)
    return pl.pallas_call(
        functools.partial(body, D // HEADS),
        grid=(rows, width // lanes),
        in_specs=[
            pl.BlockSpec((1, seq_len, 1), lambda r, h: (r, 0, 0)),
            pl.BlockSpec((1, 1, seq_len), lambda r, h: (r, 0, 0)),
        ]
        + [tile] * len(arrays),
        out_specs=[tile] * count_out,
        out_shape=[shape] * count_out,
        cost_estimate=pl.CostEstimate(
            flops=flops,
            bytes_accessed=2 * arrays[0].size * (len(arrays) + count_out),
            transcendentals=rows * HEADS * seq_len * seq_len,
        ),
    )(segment_id[:, :, None], segment_id[:, None, :], *arrays)


def per_device(
    inputs,
    cotangent,
    span_lengths,
    pad_lengths,
    pairing,
    owner_slot,
    master,
    first_moment,
    second_moment,
    left_basis,
    right_basis,
    vector_master,
    vector_first,
    vector_second,
):
    pair_count = lax.axis_size("pair")
    data_count = lax.axis_size("dp")
    grad_scale = 1.0 / (pair_count * data_count)
    block_side = master.shape[-1]
    half = block_side // pair_count
    core = lax.axis_index("pair")
    own_half = lax.dynamic_slice_in_dim(master, core * half, half, axis=1).astype(jnp.bfloat16)
    gathered = spread(own_half, data_count, pair_count)
    w_query, w_key, w_value, w_output, w_inner, w_outer = assemble(
        gathered, owner_slot, pair_count
    )
    (
        gain_one,
        shift_one,
        gain_two,
        shift_two,
        bias_query,
        bias_value,
        bias_output,
        bias_outer,
        bias_inner,
    ) = split_vector(vector_master)
    row_count = inputs.shape[1]
    seq_len = inputs.shape[2]
    token_count = row_count * seq_len
    flat_input = inputs.reshape(token_count, D)
    span_rows = span_lengths[0]
    pad_rows = pad_lengths[0]
    span_ends = jnp.cumsum(span_rows, axis=-1)
    span_starts = span_ends - span_rows
    positions = jnp.arange(seq_len, dtype=jnp.int32)
    inside = jnp.sum(
        (positions[None, :, None] >= span_ends[:, None, :-1]).astype(jnp.int32), axis=-1
    )
    segment_id = jnp.where(positions[None, :] >= seq_len - pad_rows[:, None], SEGS, inside)
    query_rows = (
        (jnp.dot(flat_input, w_query, preferred_element_type=jnp.float32) + bias_query)
        .astype(jnp.bfloat16)
    )
    key_rows = (
        jnp.dot(flat_input, w_key, preferred_element_type=jnp.float32)
        .astype(jnp.bfloat16)
    )
    value_rows = (
        (jnp.dot(flat_input, w_value, preferred_element_type=jnp.float32) + bias_value)
        .astype(jnp.bfloat16)
    )
    (mixed_low,) = attention_call(
        attend_forward_body, 1, segment_id, (query_rows, key_rows, value_rows)
    )
    branch = jnp.dot(mixed_low, w_output, preferred_element_type=jnp.float32) + bias_output
    residual_one = flat_input.astype(jnp.float32) + branch
    normed = layer_norm(residual_one, gain_one, shift_one)
    normed_low = normed.astype(jnp.bfloat16)
    inner_sum = jnp.dot(normed_low, w_inner, preferred_element_type=jnp.float32) + bias_inner
    active, slope = gelu_and_slope(inner_sum)
    active_low, slope_low = active.astype(jnp.bfloat16), slope.astype(jnp.bfloat16)
    outer_sum = jnp.dot(active_low, w_outer, preferred_element_type=jnp.float32) + bias_outer
    residual_two = normed + outer_sum
    result = layer_norm(residual_two, gain_two, shift_two)
    result_rows = result.reshape(row_count, seq_len, D)
    leaders = jnp.take_along_axis(result_rows, span_starts[:, :, None], axis=1).reshape(-1, D)
    partner = swapped(leaders.astype(jnp.bfloat16), "pair", 0).astype(jnp.float32)
    pair_logits = (
        jnp.dot(leaders, partner.T, precision=HIGHEST, preferred_element_type=jnp.float32)
        * CLS_SCALE
    )
    pair_probs = jax.nn.softmax(pair_logits, axis=-1)
    targets = (
        pairing.reshape(-1)[:, None] == jnp.arange(leaders.shape[0], dtype=jnp.int32)[None, :]
    ).astype(jnp.float32)
    grad_pair = CLS_WEIGHT * CLS_SCALE * (pair_probs - targets)
    grad_leaders = jnp.dot(
        grad_pair, partner, precision=HIGHEST, preferred_element_type=jnp.float32
    )
    grad_partner = jnp.dot(
        grad_pair.T, leaders, precision=HIGHEST, preferred_element_type=jnp.float32
    )
    returned = swapped(grad_partner.astype(jnp.bfloat16), "pair", 0).astype(jnp.float32)
    grad_leaders = grad_leaders + returned
    valid_mask = (segment_id < SEGS).astype(jnp.float32)
    grad_result = cotangent[0].astype(jnp.float32) * valid_mask[:, :, None]
    row_index = jnp.arange(row_count, dtype=jnp.int32)[:, None]
    grad_result = grad_result.at[row_index, span_starts].add(
        grad_leaders.reshape(row_count, SEGS, D)
    )
    grad_result = grad_result.reshape(token_count, D)
    primal_two, norm_two_back = jax.vjp(layer_norm, residual_two, gain_two, shift_two)
    grad_residual_two, grad_gain_two, grad_shift_two = norm_two_back(grad_result)
    grad_outer = grad_residual_two.astype(jnp.bfloat16)
    grad_bias_outer = jnp.sum(grad_outer, axis=0, dtype=jnp.float32)
    grad_w_outer = jnp.einsum(
        "tf,td->fd", active_low, grad_outer, preferred_element_type=jnp.float32
    )
    grad_active = jnp.einsum("td,fd->tf", grad_outer, w_outer, preferred_element_type=jnp.float32)
    grad_inner = (grad_active * slope_low.astype(jnp.float32)).astype(jnp.bfloat16)
    grad_bias_inner = jnp.sum(grad_inner, axis=0, dtype=jnp.float32)
    grad_w_inner = jnp.einsum(
        "td,tf->df", normed_low, grad_inner, preferred_element_type=jnp.float32
    )
    grad_normed = grad_residual_two + jnp.einsum(
        "tf,df->td", grad_inner, w_inner, preferred_element_type=jnp.float32
    )
    primal_one, norm_one_back = jax.vjp(layer_norm, residual_one, gain_one, shift_one)
    grad_residual_one, grad_gain_one, grad_shift_one = norm_one_back(grad_normed)
    grad_branch = grad_residual_one.astype(jnp.bfloat16)
    grad_bias_output = jnp.sum(grad_branch, axis=0, dtype=jnp.float32)
    grad_w_output = jnp.einsum(
        "td,te->de", mixed_low, grad_branch, preferred_element_type=jnp.float32
    )
    grad_mixed = (
        jnp.einsum("te,de->td", grad_branch, w_output, preferred_element_type=jnp.float32)
        .astype(jnp.bfloat16)
    )
    grad_query, grad_key, grad_value = attention_call(
        attend_backward_body, 3, segment_id, (query_rows, key_rows, value_rows, grad_mixed)
    )
    grad_bias_query = jnp.sum(grad_query, axis=0, dtype=jnp.float32)
    grad_bias_value = jnp.sum(grad_value, axis=0, dtype=jnp.float32)
    grad_w_query = jnp.einsum(
        "td,te->de", flat_input, grad_query, preferred_element_type=jnp.float32
    )
    grad_w_key = jnp.einsum("td,te->de", flat_input, grad_key, preferred_element_type=jnp.float32)
    grad_w_value = jnp.einsum(
        "td,te->de", flat_input, grad_value, preferred_element_type=jnp.float32
    )
    grad_inputs = grad_residual_one + jnp.einsum(
        "te,de->td", grad_query, w_query, preferred_element_type=jnp.float32
    )
    grad_inputs = grad_inputs + jnp.einsum(
        "te,de->td", grad_key, w_key, preferred_element_type=jnp.float32
    )
    grad_inputs = grad_inputs + jnp.einsum(
        "te,de->td", grad_value, w_value, preferred_element_type=jnp.float32
    )
    local_vector = (
        jnp.concatenate(
            [
                grad_gain_one,
                grad_shift_one,
                grad_gain_two,
                grad_shift_two,
                grad_bias_query,
                grad_bias_value,
                grad_bias_output,
                grad_bias_outer,
                grad_bias_inner,
            ]
        )
        * grad_scale
    )
    grad_mats = pair_summed(
        [
            (matrix * grad_scale).astype(jnp.bfloat16)
            for matrix in (
                grad_w_query, grad_w_key, grad_w_value, grad_w_output, grad_w_inner, grad_w_outer
            )
        ],
        half,
    )
    own_grad = deal(grad_mats, owner_slot, master.shape[0] * data_count, half, block_side)
    vector_grad = vector_total(local_vector, data_count, pair_count)
    own_grad = fold(own_grad, data_count, pair_count)
    owned_grad = lax.all_gather(own_grad, "pair", axis=1, tiled=True).astype(jnp.float32)
    new_master, new_first, new_second = soap_update(
        owned_grad, master, first_moment, second_moment, left_basis, right_basis
    )
    new_vector, vector_one, vector_two = adam_update(
        vector_grad, vector_master, vector_first, vector_second
    )
    return (
        result_rows.astype(jnp.bfloat16).reshape(inputs.shape),
        grad_inputs.reshape(inputs.shape),
        owned_grad,
        new_master,
        new_first,
        new_second,
        vector_grad,
        jnp.stack([new_vector, vector_one, vector_two], axis=0),
    )


def solution(mesh):
    placed = (
        P("pair", "dp", None, None),
        P("pair", "dp", None, None),
        P("pair", "dp", None),
        P("pair", "dp"),
        P("pair", "dp", None),
        P(),
        P("dp", None, None),
        P("dp", None, None),
        P("dp", None, None),
        P("dp", None, None),
        P("dp", None, None),
        P(),
        P(),
        P(),
    )
    return jax.shard_map(
        per_device,
        mesh=mesh,
        in_specs=placed,
        out_specs=(
            P("pair", "dp", None, None),
            P("pair", "dp", None, None),
            P("dp", None, None),
            P("dp", None, None),
            P("dp", None, None),
            P("dp", None, None),
            P(),
            P(),
        ),
        check_vma=False,
    )
```

```python
import functools
import math

import jax
import jax.numpy as jnp
from jax import lax
from jax.experimental import pallas as pl
from jax.experimental.pallas import tpu as pltpu
from jax.sharding import PartitionSpec as P

D = 768
HEADS = 12
FF = 3072
SEGS = 4
STEP = 10


HIGHEST = lax.Precision.HIGHEST
BETA_ONE = 0.9
BETA_TWO = 0.95
ADAM_EPS = 1e-08
LR_MATRIX = 0.1
LR_VECTOR = 1.0
DECAY_RATE = 0.01
NORM_EPS = 1e-12
CLS_SCALE = 0.0625
CLS_WEIGHT = 4.0


def swapped(array, axis, stride):
    return lax.ppermute(array, axis, [(i, i ^ 1 << stride) for i in range(lax.axis_size(axis))])


def layer_norm(values, gain_vector, shift_vector):
    average = jnp.mean(values, axis=-1, keepdims=True)
    centered = values - average
    variance = jnp.mean(centered * centered, axis=-1, keepdims=True)
    return centered * lax.rsqrt(variance + NORM_EPS) * gain_vector + shift_vector


def gelu_and_slope(values):
    lower = 0.5 * (1.0 + lax.erf(values * math.sqrt(0.5)))
    density = jnp.exp(-0.5 * values * values) * (1.0 / math.sqrt(2.0 * math.pi))
    return values * lower, lower + values * density


def split_vector(vector):
    pieces = [vector[index * D : (index + 1) * D] for index in range(8)]
    return tuple(pieces) + (vector[8 * D : 8 * D + FF],)


def matrix_shapes():
    return ((D, D),) * 4 + ((D, FF), (FF, D))


def tile_walk(block_side):
    for index, (rows, cols) in enumerate(matrix_shapes()):
        for row in range(rows // block_side):
            for col in range(cols // block_side):
                yield index, row, col


def assemble_body(per_owner, halves, slot_ref, gathered_ref, *refs):
    mats, sems = refs[:-1], refs[-1]
    half, side = gathered_ref.shape[-2:]
    for block, (index, row, col) in enumerate(tile_walk(side)):
        slot = slot_ref[block]
        owner, place = lax.div(slot, per_owner), lax.rem(slot, per_owner)
        for part in range(halves):
            pltpu.make_async_copy(
                gathered_ref.at[owner * halves + part, place],
                mats[index].at[
                    pl.ds(row * side + part * half, half), pl.ds(col * side, side)
                ],
                sems.at[index],
            ).start()
    for index, matrix in enumerate(mats):
        pltpu.make_async_copy(matrix, matrix, sems.at[index]).wait()


def assemble(gathered, owner_slot, halves):
    shapes = matrix_shapes()
    return pl.pallas_call(
        functools.partial(assemble_body, gathered.shape[1], halves),
        in_specs=[
            pl.BlockSpec(memory_space=pltpu.SMEM),
            pl.BlockSpec(memory_space=pl.ANY),
        ],
        out_specs=[pl.BlockSpec(memory_space=pltpu.VMEM)] * len(shapes),
        out_shape=[jax.ShapeDtypeStruct(shape, gathered.dtype) for shape in shapes],
        scratch_shapes=[pltpu.SemaphoreType.DMA((len(shapes),))],
        cost_estimate=pl.CostEstimate(
            flops=0, bytes_accessed=4 * gathered.size, transcendentals=0
        ),
    )(owner_slot, gathered)


def deal_body(side, slot_ref, zero_ref, *refs):
    mats, (dealt_ref, used_ref, sem) = refs[:-3], refs[-3:]
    half = dealt_ref.shape[1]

    @pl.loop(0, dealt_ref.shape[0])
    def _(slot):
        used_ref[slot] = 0

    for block, (index, row, col) in enumerate(tile_walk(side)):
        slot = slot_ref[block]
        used_ref[slot] = 1
        pltpu.make_async_copy(
            mats[index].at[pl.ds(row * half, half), pl.ds(col * side, side)],
            dealt_ref.at[slot],
            sem,
        ).start()

    @pl.loop(0, dealt_ref.shape[0])
    def _(slot):
        @pl.when(used_ref[slot] == 0)
        def _():
            pltpu.make_async_copy(zero_ref, dealt_ref.at[slot], sem).start()

    pltpu.make_async_copy(dealt_ref, dealt_ref, sem).wait()


def deal(mats, owner_slot, slot_total, half, side):
    dtype = mats[0].dtype
    return pl.pallas_call(
        functools.partial(deal_body, side),
        in_specs=[pl.BlockSpec(memory_space=pltpu.SMEM)]
        + [pl.BlockSpec(memory_space=pltpu.VMEM)] * (1 + len(mats)),
        out_specs=pl.BlockSpec(memory_space=pl.ANY),
        out_shape=jax.ShapeDtypeStruct((slot_total, half, side), dtype),
        scratch_shapes=[pltpu.SMEM((slot_total,), jnp.int32), pltpu.SemaphoreType.DMA],
        cost_estimate=pl.CostEstimate(
            flops=0, bytes_accessed=4 * slot_total * half * side, transcendentals=0
        ),
    )(owner_slot, jnp.zeros((half, side), dtype), *mats)


MESH_IDS = pl.DeviceIdType.MESH


def spread_body(own_ref, out_ref, send_sem, recv_sem, local_sem):
    core, me = lax.axis_index("pair"), lax.axis_index("dp")
    level, rest = lax.div(me, 4), lax.rem(me, 4)
    flip_y = me + 2 - 4 * lax.div(rest, 2)
    flip_x = me + 1 - 2 * lax.rem(rest, 2)
    first = (1 - core) * flip_y + core * flip_x
    second = (1 - core) * flip_x + core * flip_y
    both = flip_x + flip_y - me
    targets = (
        (core, me + 4), (core, me - 4), (core, first), (core, second), (1 - core, me)
    )

    barrier = pltpu.get_barrier_semaphore()

    def greet(kind):
        pl.semaphore_signal(barrier, inc=1, device_id=targets[kind], device_id_type=MESH_IDS)

    @pl.when(level < 3)
    def _():
        greet(0)

    @pl.when(level > 0)
    def _():
        greet(1)

    for kind in (2, 3, 4):
        greet(kind)

    pl.semaphore_wait(barrier, 3 + lax.div(level + 3, 4) + lax.div(6 - level, 4))

    def link(kind, source, piece=None):
        place = source * 2 + core
        return pltpu.make_async_remote_copy(
            src_ref=out_ref.at[place] if piece is None else piece,
            dst_ref=out_ref.at[place],
            send_sem=send_sem.at[kind, source],
            recv_sem=recv_sem.at[kind // 4, source],
            device_id=targets[kind],
            device_id_type=MESH_IDS,
        )

    def walk(act):
        def line(base, step, kinds, up=(), down=()):
            @pl.when(level >= step)
            def _():
                act(base - 4 * step, kinds, up)

            @pl.when(level + step <= 3)
            def _():
                act(base + 4 * step, kinds, down)

        line(me, 1, (3, 2, 4), (0,), (1,))
        act(first, (3, 4), ())
        line(me, 2, (3, 2, 4), (0,), (1,))
        line(first, 1, (3, 4))
        line(me, 3, (3, 2, 4), (0,), (1,))
        line(first, 2, (3, 4))
        line(first, 3, (3, 4))
        act(second, (4,), ())
        line(second, 1, (4,))
        act(both, (4,), ())
        line(second, 2, (4,))
        line(both, 1, (4,))
        line(second, 3, (4,))
        line(both, 2, (4,))
        line(both, 3, (4,))

    def guarded(kind, run):
        if kind == 0:
            pl.when(level < 3)(run)
        elif kind == 1:
            pl.when(level > 0)(run)
        else:
            run()

    def go(source, kinds, further):
        link(0, source).wait_recv()
        for kind in further + kinds:
            guarded(kind, lambda kind=kind: link(kind, source).start())

    def drain(source, kinds, further):
        for kind in further + kinds:
            guarded(kind, lambda kind=kind: link(kind, source).wait_send())

    for kind in range(5):
        guarded(kind, lambda kind=kind: link(kind, me, own_ref).start())
    local = pltpu.make_async_copy(own_ref, out_ref.at[me * 2 + core], local_sem)
    local.start()
    walk(go)
    for kind in range(5):
        guarded(kind, lambda kind=kind: link(kind, me, own_ref).wait_send())
    walk(drain)

    @pl.loop(0, 16)
    def _(source):
        pltpu.make_async_remote_copy(
            src_ref=own_ref,
            dst_ref=out_ref.at[source * 2 + 1 - core],
            send_sem=send_sem.at[4, source],
            recv_sem=recv_sem.at[1, source],
            device_id=targets[4],
            device_id_type=MESH_IDS,
        ).wait_recv()

    local.wait()


def spread(own, data_count, pair_count):
    if (data_count, pair_count) != (16, 2):
        return lax.all_gather(own, ("dp", "pair"), axis=0)
    return pl.pallas_call(
        spread_body,
        in_specs=[pl.BlockSpec(memory_space=pl.ANY)],
        out_specs=pl.BlockSpec(memory_space=pl.ANY),
        out_shape=jax.ShapeDtypeStruct((32,) + own.shape, own.dtype),
        scratch_shapes=[
            pltpu.SemaphoreType.DMA((5, 16)),
            pltpu.SemaphoreType.DMA((2, 16)),
            pltpu.SemaphoreType.DMA,
        ],
        compiler_params=pltpu.CompilerParams(collective_id=1, has_side_effects=True),
    )(own)


def fold_body(own_ref, out_ref, land, send_sem, recv_sem):
    core, me = lax.axis_index("pair"), lax.axis_index("dp")
    level, rest = lax.div(me, 4), lax.rem(me, 4)
    flip_y = me + 2 - 4 * lax.div(rest, 2)
    flip_x = me + 1 - 2 * lax.rem(rest, 2)
    first = (1 - core) * flip_y + core * flip_x
    second = (1 - core) * flip_x + core * flip_y
    both = flip_x + flip_y - me
    targets = ((core, second), (core, second), (core, first), (core, me + 4), (core, me - 4))
    barrier = pltpu.get_barrier_semaphore()

    def greet(kind):
        pl.semaphore_signal(barrier, inc=1, device_id=targets[kind], device_id_type=MESH_IDS)

    @pl.when(level < 3)
    def _():
        greet(3)

    @pl.when(level > 0)
    def _():
        greet(4)

    greet(0)
    greet(2)
    pl.semaphore_wait(barrier, 2 + lax.div(level + 3, 4) + lax.div(6 - level, 4))

    def link(kind, place, source):
        return pltpu.make_async_remote_copy(
            src_ref=source,
            dst_ref=land.at[kind, place],
            send_sem=send_sem.at[kind, place],
            recv_sem=recv_sem.at[kind, place],
            device_id=targets[kind],
            device_id_type=MESH_IDS,
        )

    def landed(kind, place):
        link(kind, place, land.at[kind, place]).wait_recv()

    def levels(step, act):
        if step == 0:
            act(level, 0)
            return

        @pl.when(level >= step)
        def _():
            act(level - step, -1)

        @pl.when(level + step <= 3)
        def _():
            act(level + step, 1)

    def column(base, place):
        return base + 4 * (place - level)

    def total(piece, place, kinds, store):
        @pl.loop(0, own_ref.shape[1])
        def _(row):
            value = own_ref[piece, row].astype(jnp.float32)
            for kind in kinds:
                value = value + land[kind, place, row].astype(jnp.float32)
            store(row, value.astype(land.dtype))

    def send_second(kind, base):
        def act(place, side):
            link(kind, place, own_ref.at[column(base, place)]).start()

        return act

    def send_first(place, side):
        landed(1, place)

        def store(row, value):
            land[1, place, row] = value

        total(column(first, place), place, (1,), store)
        link(2, place, land.at[1, place]).start()

    def send_along(place, side):
        landed(0, place)
        landed(2, place)
        kind = 3 if side > 0 else 4
        ends = level == (0 if side > 0 else 3)

        def store(row, value):
            land[0, place, row] = value

        @pl.when(ends)
        def _():
            total(column(me, place), place, (0, 2), store)

        @pl.when(jnp.logical_not(ends))
        def _():
            landed(kind, place)
            total(column(me, place), place, (0, 2, kind), store)

        link(kind, place, land.at[0, place]).start()

    for step, kind in ((3, 1), (2, 1), (3, 0), (1, 1), (2, 0), (0, 1), (1, 0), (0, 0)):
        levels(step, send_second(kind, both if kind else second))
    levels(3, send_first)
    levels(2, send_first)
    levels(3, send_along)
    levels(1, send_first)
    levels(2, send_along)
    levels(0, send_first)
    levels(1, send_along)

    def keep(row, value):
        out_ref[row] = value

    landed(0, level)
    landed(2, level)

    @pl.when(level == 0)
    def _():
        landed(4, level)
        total(me, level, (0, 2, 4), keep)

    @pl.when(level == 3)
    def _():
        landed(3, level)
        total(me, level, (0, 2, 3), keep)

    @pl.when(jnp.logical_and(level > 0, level < 3))
    def _():
        landed(3, level)
        landed(4, level)
        total(me, level, (0, 2, 3, 4), keep)

    for step in range(4):
        for kind in range(3):
            levels(step, lambda place, side, kind=kind: link(kind, place, land.at[0, 0]).wait_send())
        if step:
            levels(
                step,
                lambda place, side: link(
                    3 if side > 0 else 4, place, land.at[0, 0]
                ).wait_send(),
            )


def fold(dealt, data_count, pair_count):
    if (data_count, pair_count) != (16, 2):
        return lax.psum_scatter(dealt, "dp", scatter_dimension=0, tiled=True)
    pieces = dealt.reshape((16, dealt.shape[0] // 16) + dealt.shape[1:])
    return pl.pallas_call(
        fold_body,
        in_specs=[pl.BlockSpec(memory_space=pltpu.VMEM)],
        out_specs=pl.BlockSpec(memory_space=pltpu.VMEM),
        out_shape=jax.ShapeDtypeStruct(pieces.shape[1:], dealt.dtype),
        scratch_shapes=[
            pltpu.VMEM((5, 4) + pieces.shape[1:], dealt.dtype),
            pltpu.SemaphoreType.DMA((5, 4)),
            pltpu.SemaphoreType.DMA((5, 4)),
        ],
        compiler_params=pltpu.CompilerParams(collective_id=2, has_side_effects=True),
    )(pieces)


def pair_body(half, count, rounds, *refs):
    part_ref, mats, refs = refs[0], refs[1 : 1 + count], refs[1 + count :]
    total_ref, outs, refs = refs[0], refs[1 : 1 + count], refs[1 + count :]
    lands, refs = refs[:count], refs[count:]
    send_sem, recv_sem, own_sem, held, landed, vector_send, vector_recv = refs
    core, me = lax.axis_index("pair"), lax.axis_index("dp")
    target = (1 - core, me)
    partners = [target]
    for step in range(rounds - 1):
        bit = 2**step
        partners.append((core, me + bit - 2 * bit * lax.rem(lax.div(me, bit), 2)))
    barrier = pltpu.get_barrier_semaphore()
    for partner in partners:
        pl.semaphore_signal(barrier, inc=1, device_id=partner, device_id_type=MESH_IDS)
    pl.semaphore_wait(barrier, rounds)

    def exchange(step):
        return pltpu.make_async_remote_copy(
            src_ref=part_ref if step == 0 else held.at[step - 1],
            dst_ref=landed.at[step],
            send_sem=vector_send.at[step],
            recv_sem=vector_recv.at[step],
            device_id=partners[step],
            device_id_type=MESH_IDS,
        )

    def finish(step):
        exchange(step).wait()
        total = (part_ref[...] if step == 0 else held[step - 1]) + landed[step]
        if step < rounds - 1:
            held[step] = total
            exchange(step + 1).start()
        else:
            total_ref[...] = total

    exchange(0).start()
    stripes = []
    for index in range(count):
        for row in range(outs[index].shape[0] // half):
            number = len(stripes)
            here = pl.ds(row * half, half)

            def rows_of(part, row=row):
                return pl.ds(pl.multiple_of((2 * row + part) * half, half), half)

            remote = pltpu.make_async_remote_copy(
                src_ref=mats[index].at[rows_of(1 - core)],
                dst_ref=lands[index].at[here],
                send_sem=send_sem.at[number],
                recv_sem=recv_sem.at[number],
                device_id=target,
                device_id_type=MESH_IDS,
            )
            remote.start()
            own = pltpu.make_async_copy(
                mats[index].at[rows_of(core)], outs[index].at[here], own_sem.at[number]
            )
            own.start()
            stripes.append((index, row, remote, own))
    every = len(stripes) // (rounds + 1)
    for number, (index, row, remote, own) in enumerate(stripes):
        if number and number % every == 0 and number // every <= rounds:
            finish(number // every - 1)
        own.wait()
        remote.wait()
        out, land = outs[index], lands[index]

        @pl.loop(0, half // 16)
        def _(step, out=out, land=land, row=row):
            rows = pl.ds(pl.multiple_of(row * half + step * 16, 16), 16)
            total = out[rows, :].astype(jnp.float32) + land[rows, :].astype(jnp.float32)
            out[rows, :] = total.astype(out.dtype)


def pair_summed(vector, mats, half, device_count):
    count, rounds = len(mats), device_count.bit_length() - 1
    shapes = [(matrix.shape[0] // 2, matrix.shape[1]) for matrix in mats]
    stripes = sum(shape[0] // half for shape in shapes)
    vector_shape = (vector.shape[0] // 128, 128)
    total, *summed = pl.pallas_call(
        functools.partial(pair_body, half, count, rounds),
        in_specs=[pl.BlockSpec(memory_space=pltpu.VMEM)]
        + [pl.BlockSpec(memory_space=pl.ANY)] * count,
        out_specs=[pl.BlockSpec(memory_space=pltpu.VMEM)] * (1 + count),
        out_shape=[jax.ShapeDtypeStruct(vector_shape, vector.dtype)]
        + [jax.ShapeDtypeStruct(shape, mats[0].dtype) for shape in shapes],
        scratch_shapes=[pltpu.VMEM(shape, mats[0].dtype) for shape in shapes]
        + [pltpu.SemaphoreType.DMA((stripes,))] * 3
        + [pltpu.VMEM((rounds,) + vector_shape, vector.dtype)] * 2
        + [pltpu.SemaphoreType.DMA((rounds,))] * 2,
        compiler_params=pltpu.CompilerParams(collective_id=3, has_side_effects=True),
    )(vector.reshape(vector_shape), *mats)
    return total.reshape(-1), summed


def soap_update(gradient, weight, moment_one, moment_two, left_basis, right_basis):
    rotated = jnp.matmul(
        jnp.matmul(jnp.swapaxes(left_basis, -1, -2), gradient, precision=HIGHEST),
        right_basis,
        precision=HIGHEST,
    )
    moment_one = BETA_ONE * moment_one + (1.0 - BETA_ONE) * rotated
    moment_two = BETA_TWO * moment_two + (1.0 - BETA_TWO) * rotated * rotated
    direction = (
        moment_one
        / (1.0 - BETA_ONE**STEP)
        / (jnp.sqrt(moment_two / (1.0 - BETA_TWO**STEP)) + ADAM_EPS)
    )
    restored = jnp.matmul(
        jnp.matmul(left_basis, direction, precision=HIGHEST),
        jnp.swapaxes(right_basis, -1, -2),
        precision=HIGHEST,
    )
    return (weight - LR_MATRIX * (restored + DECAY_RATE * weight), moment_one, moment_two)


def adam_update(gradient, weight, moment_one, moment_two):
    moment_one = BETA_ONE * moment_one + (1.0 - BETA_ONE) * gradient
    moment_two = BETA_TWO * moment_two + (1.0 - BETA_TWO) * gradient * gradient
    direction = (
        moment_one
        / (1.0 - BETA_ONE**STEP)
        / (jnp.sqrt(moment_two / (1.0 - BETA_TWO**STEP)) + ADAM_EPS)
    )
    return (weight - LR_VECTOR * direction, moment_one, moment_two)


def scores_of(left, right):
    return lax.dot_general(
        left, right, (((1,), (1,)), ((), ())), preferred_element_type=jnp.float32
    )


def attend_forward_body(head_dim, seg_col, seg_row, q_ref, k_ref, v_ref, o_ref):
    allowed = seg_col[0] == seg_row[0]
    factor = 1.0 / math.sqrt(head_dim)
    for start in range(0, q_ref.shape[1], head_dim):
        lanes = slice(start, start + head_dim)
        scores = scores_of(k_ref[:, lanes], q_ref[:, lanes])
        scores = jnp.where(allowed, scores * factor, -1e30)
        top = jnp.max(scores, axis=0, keepdims=True)
        weights = jnp.exp(scores - top)
        total = jnp.sum(weights, axis=0, keepdims=True)
        probs = (weights * (1.0 / total)).astype(jnp.bfloat16)
        mixed = lax.dot_general(
            probs, v_ref[:, lanes], (((0,), (0,)), ((), ())), preferred_element_type=jnp.float32
        )
        o_ref[:, lanes] = mixed.astype(o_ref.dtype)


def attend_backward_body(
    head_dim, seg_col, seg_row, q_ref, k_ref, v_ref, g_ref, dq_ref, dk_ref, dv_ref
):
    allowed = seg_col[0] == seg_row[0]
    factor = 1.0 / math.sqrt(head_dim)
    for start in range(0, q_ref.shape[1], head_dim):
        lanes = slice(start, start + head_dim)
        query, key = q_ref[:, lanes], k_ref[:, lanes]
        value, grad = v_ref[:, lanes], g_ref[:, lanes]
        scores = jnp.where(allowed, scores_of(key, query) * factor, -1e30)
        top = jnp.max(scores, axis=0, keepdims=True)
        weights = jnp.exp(scores - top)
        total = jnp.sum(weights, axis=0, keepdims=True)
        probs = weights * (1.0 / total)
        dv = jnp.dot(probs.astype(jnp.bfloat16), grad, preferred_element_type=jnp.float32)
        dv_ref[:, lanes] = dv.astype(dv_ref.dtype)
        grad_probs = scores_of(value, grad)
        inner = jnp.sum(probs * grad_probs, axis=0, keepdims=True)
        grad_scores = probs * (grad_probs - inner)
        grad_logits = jnp.where(allowed, grad_scores * factor, 0.0).astype(jnp.bfloat16)
        dk = jnp.dot(grad_logits, query, preferred_element_type=jnp.float32)
        dk_ref[:, lanes] = dk.astype(dk_ref.dtype)
        dq = lax.dot_general(
            grad_logits, key, (((0,), (0,)), ((), ())), preferred_element_type=jnp.float32
        )
        dq_ref[:, lanes] = dq.astype(dq_ref.dtype)


def attention_call(body, count_out, segment_id, arrays):
    rows, seq_len = segment_id.shape
    width = arrays[0].shape[1]
    lanes = 2 * (D // HEADS)
    tile = pl.BlockSpec((seq_len, lanes), lambda r, h: (r, h))
    shape = jax.ShapeDtypeStruct(arrays[0].shape, jnp.bfloat16)
    flops = 2 * rows * seq_len * seq_len * width * (2 if count_out == 1 else 5)
    return pl.pallas_call(
        functools.partial(body, D // HEADS),
        grid=(rows, width // lanes),
        in_specs=[
            pl.BlockSpec((1, seq_len, 1), lambda r, h: (r, 0, 0)),
            pl.BlockSpec((1, 1, seq_len), lambda r, h: (r, 0, 0)),
        ]
        + [tile] * len(arrays),
        out_specs=[tile] * count_out,
        out_shape=[shape] * count_out,
        cost_estimate=pl.CostEstimate(
            flops=flops,
            bytes_accessed=2 * arrays[0].size * (len(arrays) + count_out),
            transcendentals=rows * HEADS * seq_len * seq_len,
        ),
    )(segment_id[:, :, None], segment_id[:, None, :], *arrays)


def per_device(
    inputs,
    cotangent,
    span_lengths,
    pad_lengths,
    pairing,
    owner_slot,
    master,
    first_moment,
    second_moment,
    left_basis,
    right_basis,
    vector_master,
    vector_first,
    vector_second,
):
    pair_count = lax.axis_size("pair")
    data_count = lax.axis_size("dp")
    grad_scale = 1.0 / (pair_count * data_count)
    block_side = master.shape[-1]
    half = block_side // pair_count
    core = lax.axis_index("pair")
    own_half = lax.dynamic_slice_in_dim(master, core * half, half, axis=1).astype(jnp.bfloat16)
    gathered = spread(own_half, data_count, pair_count)
    w_query, w_key, w_value, w_output, w_inner, w_outer = assemble(
        gathered, owner_slot, pair_count
    )
    (
        gain_one,
        shift_one,
        gain_two,
        shift_two,
        bias_query,
        bias_value,
        bias_output,
        bias_outer,
        bias_inner,
    ) = split_vector(vector_master)
    row_count = inputs.shape[1]
    seq_len = inputs.shape[2]
    token_count = row_count * seq_len
    flat_input = inputs.reshape(token_count, D)
    span_rows = span_lengths[0]
    pad_rows = pad_lengths[0]
    span_ends = jnp.cumsum(span_rows, axis=-1)
    span_starts = span_ends - span_rows
    positions = jnp.arange(seq_len, dtype=jnp.int32)
    inside = jnp.sum(
        (positions[None, :, None] >= span_ends[:, None, :-1]).astype(jnp.int32), axis=-1
    )
    segment_id = jnp.where(positions[None, :] >= seq_len - pad_rows[:, None], SEGS, inside)
    query_rows = (
        (jnp.dot(flat_input, w_query, preferred_element_type=jnp.float32) + bias_query)
        .astype(jnp.bfloat16)
    )
    key_rows = (
        jnp.dot(flat_input, w_key, preferred_element_type=jnp.float32)
        .astype(jnp.bfloat16)
    )
    value_rows = (
        (jnp.dot(flat_input, w_value, preferred_element_type=jnp.float32) + bias_value)
        .astype(jnp.bfloat16)
    )
    (mixed_low,) = attention_call(
        attend_forward_body, 1, segment_id, (query_rows, key_rows, value_rows)
    )
    branch = jnp.dot(mixed_low, w_output, preferred_element_type=jnp.float32) + bias_output
    residual_one = flat_input.astype(jnp.float32) + branch
    normed = layer_norm(residual_one, gain_one, shift_one)
    normed_low = normed.astype(jnp.bfloat16)
    inner_sum = jnp.dot(normed_low, w_inner, preferred_element_type=jnp.float32) + bias_inner
    active, slope = gelu_and_slope(inner_sum)
    active_low, slope_low = active.astype(jnp.bfloat16), slope.astype(jnp.bfloat16)
    outer_sum = jnp.dot(active_low, w_outer, preferred_element_type=jnp.float32) + bias_outer
    residual_two = normed + outer_sum
    result = layer_norm(residual_two, gain_two, shift_two)
    result_rows = result.reshape(row_count, seq_len, D)
    leaders = jnp.take_along_axis(result_rows, span_starts[:, :, None], axis=1).reshape(-1, D)
    partner = swapped(leaders.astype(jnp.bfloat16), "pair", 0).astype(jnp.float32)
    pair_logits = (
        jnp.dot(leaders, partner.T, precision=HIGHEST, preferred_element_type=jnp.float32)
        * CLS_SCALE
    )
    pair_probs = jax.nn.softmax(pair_logits, axis=-1)
    targets = (
        pairing.reshape(-1)[:, None] == jnp.arange(leaders.shape[0], dtype=jnp.int32)[None, :]
    ).astype(jnp.float32)
    grad_pair = CLS_WEIGHT * CLS_SCALE * (pair_probs - targets)
    grad_leaders = jnp.dot(
        grad_pair, partner, precision=HIGHEST, preferred_element_type=jnp.float32
    )
    grad_partner = jnp.dot(
        grad_pair.T, leaders, precision=HIGHEST, preferred_element_type=jnp.float32
    )
    returned = swapped(grad_partner.astype(jnp.bfloat16), "pair", 0).astype(jnp.float32)
    grad_leaders = grad_leaders + returned
    valid_mask = (segment_id < SEGS).astype(jnp.float32)
    grad_result = cotangent[0].astype(jnp.float32) * valid_mask[:, :, None]
    row_index = jnp.arange(row_count, dtype=jnp.int32)[:, None]
    grad_result = grad_result.at[row_index, span_starts].add(
        grad_leaders.reshape(row_count, SEGS, D)
    )
    grad_result = grad_result.reshape(token_count, D)
    primal_two, norm_two_back = jax.vjp(layer_norm, residual_two, gain_two, shift_two)
    grad_residual_two, grad_gain_two, grad_shift_two = norm_two_back(grad_result)
    grad_outer = grad_residual_two.astype(jnp.bfloat16)
    grad_bias_outer = jnp.sum(grad_outer, axis=0, dtype=jnp.float32)
    grad_w_outer = jnp.einsum(
        "tf,td->fd", active_low, grad_outer, preferred_element_type=jnp.float32
    )
    grad_active = jnp.einsum("td,fd->tf", grad_outer, w_outer, preferred_element_type=jnp.float32)
    grad_inner = (grad_active * slope_low.astype(jnp.float32)).astype(jnp.bfloat16)
    grad_bias_inner = jnp.sum(grad_inner, axis=0, dtype=jnp.float32)
    grad_w_inner = jnp.einsum(
        "td,tf->df", normed_low, grad_inner, preferred_element_type=jnp.float32
    )
    grad_normed = grad_residual_two + jnp.einsum(
        "tf,df->td", grad_inner, w_inner, preferred_element_type=jnp.float32
    )
    primal_one, norm_one_back = jax.vjp(layer_norm, residual_one, gain_one, shift_one)
    grad_residual_one, grad_gain_one, grad_shift_one = norm_one_back(grad_normed)
    grad_branch = grad_residual_one.astype(jnp.bfloat16)
    grad_bias_output = jnp.sum(grad_branch, axis=0, dtype=jnp.float32)
    grad_w_output = jnp.einsum(
        "td,te->de", mixed_low, grad_branch, preferred_element_type=jnp.float32
    )
    grad_mixed = (
        jnp.einsum("te,de->td", grad_branch, w_output, preferred_element_type=jnp.float32)
        .astype(jnp.bfloat16)
    )
    grad_query, grad_key, grad_value = attention_call(
        attend_backward_body, 3, segment_id, (query_rows, key_rows, value_rows, grad_mixed)
    )
    grad_bias_query = jnp.sum(grad_query, axis=0, dtype=jnp.float32)
    grad_bias_value = jnp.sum(grad_value, axis=0, dtype=jnp.float32)
    grad_w_query = jnp.einsum(
        "td,te->de", flat_input, grad_query, preferred_element_type=jnp.float32
    )
    grad_w_key = jnp.einsum("td,te->de", flat_input, grad_key, preferred_element_type=jnp.float32)
    grad_w_value = jnp.einsum(
        "td,te->de", flat_input, grad_value, preferred_element_type=jnp.float32
    )
    grad_inputs = grad_residual_one + jnp.einsum(
        "te,de->td", grad_query, w_query, preferred_element_type=jnp.float32
    )
    grad_inputs = grad_inputs + jnp.einsum(
        "te,de->td", grad_key, w_key, preferred_element_type=jnp.float32
    )
    grad_inputs = grad_inputs + jnp.einsum(
        "te,de->td", grad_value, w_value, preferred_element_type=jnp.float32
    )
    local_vector = (
        jnp.concatenate(
            [
                grad_gain_one,
                grad_shift_one,
                grad_gain_two,
                grad_shift_two,
                grad_bias_query,
                grad_bias_value,
                grad_bias_output,
                grad_bias_outer,
                grad_bias_inner,
            ]
        )
        * grad_scale
    )
    vector_grad, grad_mats = pair_summed(
        local_vector,
        [
            (matrix * grad_scale).astype(jnp.bfloat16)
            for matrix in (
                grad_w_query, grad_w_key, grad_w_value, grad_w_output, grad_w_inner, grad_w_outer
            )
        ],
        half,
        pair_count * data_count,
    )
    own_grad = deal(grad_mats, owner_slot, master.shape[0] * data_count, half, block_side)
    own_grad = fold(own_grad, data_count, pair_count)
    owned_grad = lax.all_gather(own_grad, "pair", axis=1, tiled=True).astype(jnp.float32)
    new_master, new_first, new_second = soap_update(
        owned_grad, master, first_moment, second_moment, left_basis, right_basis
    )
    new_vector, vector_one, vector_two = adam_update(
        vector_grad, vector_master, vector_first, vector_second
    )
    return (
        result_rows.astype(jnp.bfloat16).reshape(inputs.shape),
        grad_inputs.reshape(inputs.shape),
        owned_grad,
        new_master,
        new_first,
        new_second,
        vector_grad,
        jnp.stack([new_vector, vector_one, vector_two], axis=0),
    )


def solution(mesh):
    placed = (
        P("pair", "dp", None, None),
        P("pair", "dp", None, None),
        P("pair", "dp", None),
        P("pair", "dp"),
        P("pair", "dp", None),
        P(),
        P("dp", None, None),
        P("dp", None, None),
        P("dp", None, None),
        P("dp", None, None),
        P("dp", None, None),
        P(),
        P(),
        P(),
    )
    return jax.shard_map(
        per_device,
        mesh=mesh,
        in_specs=placed,
        out_specs=(
            P("pair", "dp", None, None),
            P("pair", "dp", None, None),
            P("dp", None, None),
            P("dp", None, None),
            P("dp", None, None),
            P("dp", None, None),
            P(),
            P(),
        ),
        check_vma=False,
    )
```
